256 devices in a mesh: state: 256 (over y, z, x, core).
Axes of the slice: x: 4, y: 4, z: 8, core: 2. Of those that a mesh axis runs over, the one named last changes fastest.
Arguments:
- transitions: float32 [4096, 16, 4096], P('state'), may hold values from 0 to 1, as said below
- costs: float32 [4096, 16, 128], P('state'), may hold values from 0 to 4
- valid_counts: int32 [4096], P('state'), may hold values from 1 to 16
- start_values: float32 [4096, 128], P('state'), may hold values from -12 to 12
- ref_state: int32 [1], replicated, may hold values from 0 to 4095
Outputs:
- relative_values: float32 [4096, 128], P('state')
- lower_bounds: float32 [4, 128], replicated
- upper_bounds: float32 [4, 128], replicated
The draws below stay inside these ranges and needn't reach their ends.
Inputs may be any that keep to these rules, and one draw needn't show every extreme that they name: Every entry is nonnegative and each row transitions[s, a, :] sums to one up to float32 rounding. Actions 0 to valid_counts[s] - 1 are allowed in state s.
All inputs are finite; a program needn't handle non-finite values.
Results may differ from the reference program's by a relative error of at most 0.00017.
Values sent between devices are 32-bit elements; how exact they have to be, the bound alone decides.
A program may use at most 64 MiB of HBM per device.

```python
import jax
import jax.numpy as jnp
from jax import lax

STATES = 4096
ACTIONS = 16
SCENARIOS = 128
ITERS = 4


def draw_transitions(key, part):
    sigma = 2.0
    raw = jnp.exp(sigma * jax.random.normal(key, (STATES, ACTIONS, STATES), jnp.float32))
    return raw / jnp.sum(raw, axis=2, keepdims=True)


def place_ends(values, stream_key, low, top_value):
    extent = values.shape
    index_at = [jax.random.randint(jax.random.fold_in(stream_key, axis), (), 0, extent[axis]) for axis in range(len(extent))]
    values = values.at[tuple(index_at)].set(low)
    longest = extent.index(max(extent))
    index_at[longest] = (index_at[longest] + 1) % extent[longest]
    return values.at[tuple(index_at)].set(top_value)


def level_of(stream_key, dims, cuts, low, largest):
    def one(position, blocks):
        steps = jax.random.uniform(jax.random.fold_in(jax.random.fold_in(stream_key, 6), position), (blocks,), jnp.float32, low / len(cuts), largest / len(cuts))
        return jnp.repeat(jnp.exp(steps), dims[position] // blocks).reshape((-1,) + (1,) * (len(dims) - position - 1))

    factor_of = one(*cuts[0])
    for cut in cuts[1:]:
        factor_of = factor_of * one(*cut)
    return factor_of


def normal_values(stream_key, dims, deviation, bound, shards=(), held_as=jnp.bfloat16):
    loudness = level_of(stream_key, dims, shards, -0.22, 0.18) if shards else 1.0
    values = jax.random.normal(stream_key, dims, jnp.float32) * deviation * loudness
    return jnp.minimum(jnp.maximum(values, -bound), bound).astype(held_as)


def setup_inputs(seed: int = 0) -> dict:
    streams_of = jax.random.split(jax.random.key(seed), 6)
    return {
        "transitions": draw_transitions(jax.random.fold_in(streams_of[5], 71), 0),
        "costs": jnp.clip(4.0 * jax.random.uniform(streams_of[1], (STATES, ACTIONS, SCENARIOS), jnp.float32) ** level_of(streams_of[1], (STATES, ACTIONS, SCENARIOS), ((0, 256),), -0.2, 0.2), 0.0, 4.0),
        "valid_counts": place_ends(jax.random.randint(streams_of[2], (STATES,), 1, ACTIONS + 1), jax.random.fold_in(streams_of[2], 1), 1, ACTIONS).astype(jnp.int32),
        "start_values": normal_values(streams_of[3], (STATES, SCENARIOS), 2.0, 12.0, ((0, 256),), jnp.float32),
        "ref_state": jax.random.randint(streams_of[4], (1,), 0, STATES).astype(jnp.int32),
    }


big_value = 1e30


def reference(transitions, costs, valid_counts, start_values, ref_state):
    flat_rows = transitions.reshape(STATES * ACTIONS, STATES)
    allowed = jnp.arange(ACTIONS, dtype=jnp.int32)[None, :] < valid_counts[:, None]
    relative = start_values
    lower_list = []
    upper_list = []
    for iteration in range(ITERS):
        expected = jnp.dot(flat_rows, relative, precision=lax.Precision.HIGHEST, preferred_element_type=jnp.float32)
        q_values = costs + expected.reshape(STATES, ACTIONS, SCENARIOS)
        q_values = jnp.where(allowed[:, :, None], q_values, jnp.float32(big_value))
        best_value = jnp.min(q_values, axis=1)
        increase = best_value - relative
        lower_list.append(jnp.min(increase, axis=0))
        upper_list.append(jnp.max(increase, axis=0))
        ref_row = lax.dynamic_slice_in_dim(best_value, ref_state[0].astype(jnp.int32), 1, 0)
        relative = best_value - ref_row
    return relative, jnp.stack(lower_list), jnp.stack(upper_list)
```

```python
import functools

import jax
import jax.numpy as jnp
from jax import lax
from jax.experimental import pallas as pl
from jax.experimental.pallas import tpu as pltpu
from jax.sharding import Mesh
from jax.sharding import PartitionSpec as P

ITERS = 4
YS, ZS, XS = 4, 8, 4
AXES = ("y", "z", "x", "c")
BIG = 1e30
MESH = pl.DeviceIdType.MESH


def ring(delta, size):
    return min(delta, size - delta)


PLANE = sorted(
    ((da, dz) for da in range(4) for dz in range(ZS) if da or dz),
    key=lambda d: (ring(d[0], 4) + ring(d[1], ZS), ring(d[1], ZS), d),
)
GROUPS = (0, 1, 3, 2)


def kernel(
    trans,
    costs,
    counts,
    start,
    ref_state,
    rel_out,
    low_out,
    up_out,
    values,
    raw,
    hi,
    lo,
    masked,
    cost2,
    right,
    total,
    swap,
    mine,
    plane_in,
    line_in,
    half_in,
    best_io,
    plane_recv,
    line_recv,
    plane_send,
    line_send,
    raw_sem,
    raw_send,
    raw_recv,
    pair_send,
    pair_recv,
):
    y, z, x, c = (lax.axis_index(a) for a in AXES)
    a = y + c * (x - y)
    b = x + c * (y - x)

    def wrap(i, size):
        return lax.rem(i + size, size)

    def place(a_, z_, b_):
        y_ = a_ + c * (b_ - a_)
        x_ = b_ + c * (a_ - b_)
        return y_, z_, x_

    partner = (y, z, x, 1 - c)

    quarter = 64
    loads = []
    for i in range(4):
        rows = pl.ds(i * quarter, quarter)
        copy = pltpu.make_async_copy(trans.at[rows], raw.at[0, rows], raw_sem.at[i])
        copy.start()
        loads.append(copy)

    barrier = pltpu.get_barrier_semaphore()
    for da, dz in PLANE:
        pl.semaphore_signal(
            barrier, inc=1, device_id=(*place(wrap(a + da, 4), wrap(z + dz, ZS), b), c), device_id_type=MESH
        )
    for db in (1, 3, 2):
        pl.semaphore_signal(
            barrier, inc=1, device_id=(*place(a, z, wrap(b + db, 4)), c), device_id_type=MESH
        )
    pl.semaphore_signal(barrier, inc=1, device_id=partner, device_id_type=MESH)

    lane = lax.broadcasted_iota(jnp.int32, (16, 128), 1)
    left = lane < 64
    action = lax.broadcasted_iota(jnp.int32, (16, 128), 0)
    for s in range(16):
        rows = pl.ds(s * 16, 16)
        masked[0, rows, :] = jnp.where(action < counts[s], costs[rows, :], jnp.float32(BIG))

    pl.semaphore_wait(barrier, len(PLANE) + 4)

    def to_partner(src, dst, k):
        copy = pltpu.make_async_remote_copy(
            src, dst, pair_send.at[k], pair_recv.at[k], device_id=partner, device_id_type=MESH
        )
        copy.start()
        return copy

    send_start = to_partner(start, swap.at[0], 0)
    send_cost = to_partner(masked.at[0], masked.at[1], 1)
    exchanges = []
    for i in range(4):
        rows = pl.ds(i * quarter, quarter)
        copy = pltpu.make_async_remote_copy(
            trans.at[rows],
            raw.at[1, rows],
            raw_send.at[i],
            raw_recv.at[i],
            device_id=partner,
            device_id_type=MESH,
        )
        copy.start()
        exchanges.append(copy)

    keep = jnp.logical_xor(left, c == 1)

    def both_halves(v):
        return jnp.where(keep[: v.shape[0]], v, pltpu.roll(v, 64, 1))

    send_start.wait_recv()
    own = both_halves(start[...])
    other = both_halves(swap[0])
    first = jnp.where(c == 0, own, other)
    second = jnp.where(c == 0, other, own)
    values[0, y, z, x] = jnp.where(left, first, second)

    def split_rows(which, base):
        def step(i, _):
            rows = pl.ds(pl.multiple_of(i * 16, 16), 16)
            out_rows = pl.ds(pl.multiple_of(base + i * 16, 16), 16)
            for g in range(4):
                v = raw[which, rows, g * 1024 : (g + 1) * 1024]
                h = v.astype(jnp.bfloat16)
                hi[g, out_rows, :] = h
                lo[g, out_rows, :] = (v - h.astype(jnp.float32)).astype(jnp.bfloat16)
            return 0

        lax.fori_loop(0, 16, step, 0)

    def scatter_plane(t):
        src = values.at[t, y, z, x]
        for da, dz in PLANE:
            pltpu.make_async_remote_copy(
                src,
                values.at[t, y, z, x],
                plane_send.at[t],
                plane_recv.at[t, da, dz],
                device_id=(*place(wrap(a + da, 4), wrap(z + dz, ZS), b), c),
                device_id_type=MESH,
            ).start()

    def forward(t, chunk, slab):
        for db in (2, 1, 3):
            pltpu.make_async_remote_copy(
                values.at[t, *chunk],
                values.at[t, *chunk],
                line_send.at[t],
                line_recv.at[t, db, slab],
                device_id=(*place(a, z, wrap(b + db, 4)), c),
                device_id_type=MESH,
            ).start()

    def relay(t):
        forward(t, (y, z, x), 0)
        for da, dz in PLANE:
            chunk = place(wrap(a - da, 4), wrap(z - dz, ZS), b)
            pltpu.make_async_remote_copy(
                values.at[t, *chunk],
                values.at[t, *chunk],
                plane_send.at[t],
                plane_recv.at[t, da, dz],
                device_id=partner,
                device_id_type=MESH,
            ).wait_recv()
            forward(t, chunk, (4 - da) % 4)

    def wait_slab(t, db, da):
        ref = values.at[t, 0, :, 0]
        pltpu.make_async_copy(ref, ref, line_recv.at[t, db, da]).wait()

    def multiply(t, g, base, first_group):
        y_ = wrap(y + g, 4)
        v = values[t, y_].reshape(32 * 16, 128) - base
        h = v.astype(jnp.bfloat16).astype(jnp.float32)
        r = v - h
        l_ = lax.broadcasted_iota(jnp.int32, v.shape, 1) < 64
        turned = pltpu.roll(jnp.where(l_, r, h), 64, 1)
        top = jnp.where(l_, h, turned).astype(jnp.bfloat16).reshape(32, 1, 16, 128)
        bottom = jnp.where(l_, turned, r).astype(jnp.bfloat16).reshape(32, 1, 16, 128)
        right[...] = jnp.concatenate([top, bottom], axis=1).reshape(1024, 128)
        w = right[...]
        part = jnp.dot(hi[y_], w, preferred_element_type=jnp.float32)
        part += jnp.dot(lo[y_], w, preferred_element_type=jnp.float32)
        if first_group:
            total[...] = part
        else:
            total[...] += part

    def finish_costs():
        send_cost.wait_recv()

        def step(i, _):
            for which in range(2):
                rows = pl.ds(pl.multiple_of(i * 16, 16), 16)
                base = (c if which == 0 else 1 - c) * 256
                cost2[pl.ds(pl.multiple_of(base + i * 16, 16), 16), :] = both_halves(masked[which, rows, :])
            return 0

        lax.fori_loop(0, 16, step, 0)

    mine[0] = jnp.full((8, 128), -BIG, jnp.float32)
    row8 = lax.broadcasted_iota(jnp.int32, (8, 128), 0)
    lane8 = lax.broadcasted_iota(jnp.int32, (8, 128), 1)

    def iteration(t, _):
        scatter_plane(t)

        @pl.when(t == 0)
        def _():
            for copy in loads:
                copy.wait()
            split_rows(0, c * 256)

        relay(t)

        @pl.when(t == 0)
        def _():
            finish_costs()
            for copy in exchanges:
                copy.wait_recv()
            split_rows(1, (1 - c) * 256)

        packed = values[t, y, z, x]
        base = packed[0:1, :]
        base = jnp.where(lax.broadcasted_iota(jnp.int32, (1, 128), 1) < 64, base, pltpu.roll(base, 64, 1))

        for k, g in enumerate(GROUPS):

            @pl.when(c == 0)
            def _():
                for db in (1, 3, 2):
                    wait_slab(t, db, g)

            if g:

                @pl.when(c == 1)
                def _():
                    for da in range(4):
                        wait_slab(t, 4 - g, da)

            multiply(t, g, base, k == 0)

        e = total[...]
        q = e + pltpu.roll(e, 64, 1) + cost2[...]
        best = jnp.min(q.reshape(32, 16, 128), axis=1) + base
        best_io[0] = best[:16]
        best_io[1] = best[16:]
        new = jnp.where(left, best[:16], best[16:])
        values[t + 1, y, z, x] = new
        inc = new - packed
        up = jnp.max(inc, axis=0, keepdims=True)
        down = jnp.max(-inc, axis=0, keepdims=True)
        up = jnp.maximum(up, pltpu.roll(up, 64, 1))
        down = jnp.maximum(down, pltpu.roll(down, 64, 1))
        mine[0] = jnp.where(row8 == t, jnp.where(lane8 < 64, up, down), mine[0])

        chunks = values.at[t, :, :, 0]
        pltpu.make_async_copy(chunks, chunks, line_send.at[t]).wait()
        pltpu.make_async_copy(chunks, chunks, line_send.at[t]).wait()
        pltpu.make_async_copy(chunks, chunks, line_send.at[t]).wait()
        for part in (values.at[t, 0:3, :, 0], values.at[t, 0, 0:7, 0]):
            pltpu.make_async_copy(part, part, plane_send.at[t]).wait()
        return 0

    lax.fori_loop(0, ITERS, iteration, 0)

    device = (y * ZS + z) * XS + x
    ids = device * 32 + lax.broadcasted_iota(jnp.int32, (16, 128), 0)
    picked = jnp.maximum(
        jnp.where(ids == ref_state[0], best_io[0], -BIG), jnp.where(ids + 16 == ref_state[0], best_io[1], -BIG)
    )
    ref_row = jnp.max(picked, axis=0, keepdims=True)
    mine[0] = jnp.where(row8 == 4, ref_row, mine[0])
    send_best = to_partner(best_io.at[1 - c], swap.at[1], 2)

    for da, dz in PLANE:
        pltpu.make_async_remote_copy(
            mine.at[0],
            plane_in.at[da, dz],
            plane_send.at[4],
            plane_recv.at[4, da, dz],
            device_id=(*place(wrap(a + da, 4), wrap(z + dz, ZS), b), c),
            device_id_type=MESH,
        ).start()
    top = mine[0]
    for da, dz in PLANE:
        pltpu.make_async_remote_copy(
            mine.at[0],
            plane_in.at[da, dz],
            plane_send.at[4],
            plane_recv.at[4, da, dz],
            device_id=partner,
            device_id_type=MESH,
        ).wait_recv()
        top = jnp.maximum(top, plane_in[da, dz])
    mine[1] = top
    lines = []
    for db in (2, 1, 3):
        copy = pltpu.make_async_remote_copy(
            mine.at[1],
            line_in.at[db],
            line_send.at[4],
            line_recv.at[4, db, 0],
            device_id=(*place(a, z, wrap(b + db, 4)), c),
            device_id_type=MESH,
        )
        copy.start()
        lines.append((copy, db))
    for copy, db in lines:
        copy.wait_recv()
        top = jnp.maximum(top, line_in[db])
    half_in[0] = top
    send_half = to_partner(half_in.at[0], half_in.at[1], 3)
    send_half.wait_recv()
    other = half_in[1]
    r0 = jnp.where(c == 0, top, other)
    r1 = jnp.where(c == 0, other, top)
    left8 = lane8 < 64
    upper = jnp.where(left8, r0, pltpu.roll(r1, 64, 1))
    lower = -jnp.where(left8, pltpu.roll(r0, 64, 1), r1)
    ref_full = jnp.where(left8, r0, r1)[4:5]
    up_out[...] = upper[0:4]
    low_out[...] = lower[0:4]
    send_best.wait_recv()
    rel_out[...] = jnp.where(keep, jnp.where(c == 0, best_io[0], best_io[1]), swap[1]) - ref_full

    part = plane_in.at[0:3]
    pltpu.make_async_copy(part, part, plane_send.at[4]).wait()
    part = plane_in.at[0, 0:7]
    pltpu.make_async_copy(part, part, plane_send.at[4]).wait()
    part = line_in.at[0:3]
    pltpu.make_async_copy(part, part, line_send.at[4]).wait()
    for copy in (send_start, send_cost, send_best, send_half, *exchanges):
        copy.wait_send()


def local(transitions, costs, valid_counts, start_values, ref_state):
    dma = pltpu.SemaphoreType.DMA
    f32, bf16 = jnp.float32, jnp.bfloat16
    vmem = pl.BlockSpec(memory_space=pltpu.VMEM)
    smem = pl.BlockSpec(memory_space=pltpu.SMEM)
    return pl.pallas_call(
        kernel,
        out_shape=(
            jax.ShapeDtypeStruct((16, 128), f32),
            jax.ShapeDtypeStruct((ITERS, 128), f32),
            jax.ShapeDtypeStruct((ITERS, 128), f32),
        ),
        in_specs=[pl.BlockSpec(memory_space=pl.ANY), vmem, smem, vmem, smem],
        out_specs=(vmem, vmem, vmem),
        scratch_shapes=[
            pltpu.VMEM((ITERS + 1, YS, ZS, XS, 16, 128), f32),
            pltpu.VMEM((2, 256, 4096), f32),
            pltpu.VMEM((4, 512, 1024), bf16),
            pltpu.VMEM((4, 512, 1024), bf16),
            pltpu.VMEM((2, 256, 128), f32),
            pltpu.VMEM((512, 128), f32),
            pltpu.VMEM((1024, 128), bf16),
            pltpu.VMEM((512, 128), f32),
            pltpu.VMEM((2, 16, 128), f32),
            pltpu.VMEM((2, 8, 128), f32),
            pltpu.VMEM((4, ZS, 8, 128), f32),
            pltpu.VMEM((4, 8, 128), f32),
            pltpu.VMEM((2, 8, 128), f32),
            pltpu.VMEM((2, 16, 128), f32),
            dma((ITERS + 1, 4, ZS)),
            dma((ITERS + 1, 4, 4)),
            dma((ITERS + 1,)),
            dma((ITERS + 1,)),
            dma((4,)),
            dma((4,)),
            dma((4,)),
            dma((4,)),
            dma((4,)),
        ],
        compiler_params=pltpu.CompilerParams(
            collective_id=0, has_side_effects=True, vmem_limit_bytes=60 * 1024 * 1024
        ),
        name="value_iteration",
    )(
        transitions.reshape(256, 4096),
        costs.reshape(256, 128),
        valid_counts,
        start_values,
        ref_state,
    )


def solution(mesh):
    split = Mesh(mesh.devices.reshape(YS, ZS, XS, 2), AXES)
    return jax.shard_map(
        local,
        mesh=split,
        in_specs=(P(AXES, None, None), P(AXES, None, None), P(AXES), P(AXES, None), P()),
        out_specs=(P(AXES, None), P(), P()),
        check_vma=False,
    )
```

```python
import functools

import jax
import jax.numpy as jnp
from jax import lax
from jax.experimental import pallas as pl
from jax.experimental.pallas import tpu as pltpu
from jax.sharding import Mesh
from jax.sharding import PartitionSpec as P

ITERS = 4
YS, ZS, XS = 4, 8, 4
AXES = ("y", "z", "x", "c")
BIG = 1e30
MESH = pl.DeviceIdType.MESH


def ring(delta, size):
    return min(delta, size - delta)


PLANE = sorted(
    ((da, dz) for da in range(4) for dz in range(ZS) if da or dz),
    key=lambda d: (ring(d[0], 4) + ring(d[1], ZS), ring(d[1], ZS), d),
)

TREE = (
    (0, (31, 32, 12, 25, 21, 20, 7, 4, 19, 91, 99, 105, 89, 34, 58, 28, 35, 40, 1, 96, 72, 125, 92, 107, 42, 3, 70, 100, 98, 2, 127)),
    (32, (64, 67, 63, 37, 65)),
    (4, (9, 38, 36, 69, 5, 102)),
    (28, (29, 60, 124)),
    (96, (97,)),
    (31, (26, 27, 95, 126, 30)),
    (7, (71, 10, 39, 6, 103, 11)),
    (1, (33,)),
    (99, (111,)),
    (12, (14, 44, 8, 15, 108, 13)),
    (100, (68,)),
    (20, (120, 24, 23, 56, 119, 55, 116, 16, 52)),
    (40, (41, 43)),
    (92, (88, 84)),
    (105, (109, 73, 106, 101, 110, 104, 113, 74)),
    (34, (66, 62, 94)),
    (21, (22, 117, 53, 54, 17, 118)),
    (72, (75, 77, 76)),
    (91, (79, 90, 59, 87, 123, 86, 80)),
    (89, (93, 85, 122, 81, 121, 57)),
    (19, (18, 112, 115, 51, 82, 49, 114, 48, 83)),
    (42, (78, 50, 47, 46)),
    (60, (61,)),
    (44, (45,)),
)
GROUPS = (
    (
        ((0, 0), (0, 1), (1, 0), (0, 7), (3, 0), (1, 1), (0, 6), (3, 7)),
        ((0, 2), (2, 7), (0, 5), (3, 6), (2, 0), (1, 7), (0, 3), (1, 6)),
        ((2, 2), (2, 6), (3, 2), (3, 3), (1, 5), (1, 3), (0, 4), (2, 1)),
        ((2, 3), (3, 1), (1, 2), (1, 4)),
        ((2, 4), (3, 4), (2, 5), (3, 5)),
    ),
    (
        ((0, 0), (0, 1), (1, 0), (3, 0), (1, 1), (0, 7), (1, 7), (2, 7)),
        ((2, 0), (3, 7), (0, 6), (3, 6), (1, 6), (0, 2), (0, 3), (0, 5)),
        ((1, 2), (1, 3), (2, 6), (2, 1), (3, 3), (3, 2), (2, 3), (3, 1)),
        ((2, 2), (1, 4), (2, 4), (0, 4)),
        ((1, 5), (3, 4), (2, 5), (3, 5)),
    ),
)


def parts(d):
    return d // 32, d // 4 % ZS, d % 4


def step(d, p):
    return tuple((i - j) % n for i, j, n in zip(parts(d), parts(p), (4, ZS, 4)))


HOLDERS = {p: i for i, (p, _) in enumerate(TREE)}
LINE = ((0, 0, 2), (0, 0, 1), (0, 0, 3))
PARTNERS = sorted(
    {step(d, p) for p, receivers in TREE for d in receivers} | {(da, dz, 0) for da, dz in PLANE} | set(LINE)
)
PARTNERS = sorted(set(PARTNERS) | {tuple(-i % n for i, n in zip(e, (4, ZS, 4))) for e in PARTNERS})


def group_of(d, c):
    a, z, b = step(0, d)
    block = (a if c == 0 else b, z)
    return next(i for i, g in enumerate(GROUPS[c]) if block in g)


LEAVES = [d for d in range(1, 128) if d not in HOLDERS]


def kernel(
    trans,
    costs_in,
    counts_in,
    start_in,
    ref_in,
    out,
    values,
    costs,
    counts,
    start,
    ref_state,
    raw,
    hi,
    lo,
    masked,
    cost2,
    total,
    swap,
    mine,
    plane_in,
    line_in,
    half_in,
    best_io,
    hold_recv,
    leaf_recv,
    plane_recv,
    line_recv,
    send_sem,
    line_send,
    small_sem,
    raw_sem,
    raw_send,
    raw_recv,
    pair_send,
    pair_recv,
):
    y, z, x, c = (lax.axis_index(a) for a in AXES)
    a = y + c * (x - y)
    b = x + c * (y - x)

    def wrap(i, size):
        return lax.rem(i + size, size)

    def place(a_, z_, b_):
        y_ = a_ + c * (b_ - a_)
        x_ = b_ + c * (a_ - b_)
        return y_, z_, x_

    partner = (y, z, x, 1 - c)
    here = (y * ZS + z) * XS + x

    def member(da, dz, db):
        return (*place(wrap(a + da, 4), wrap(z + dz, ZS), wrap(b + db, 4)), c)

    def source(d):
        da, dz, db = parts(d)
        y_, z_, x_ = place(wrap(a - da, 4), wrap(z - dz, ZS), wrap(b - db, 4))
        return (y_ * ZS + z_) * XS + x_

    small = []
    for i, (src, dst) in enumerate(
        ((start_in, start), (costs_in, costs), (counts_in, counts), (ref_in, ref_state))
    ):
        copy = pltpu.make_async_copy(src, dst, small_sem.at[i])
        copy.start()
        small.append(copy)
    quarter = 64
    loads = []
    for i in range(4):
        rows = pl.ds(i * quarter, quarter)
        copy = pltpu.make_async_copy(trans.at[rows], raw.at[0, rows], raw_sem.at[i])
        copy.start()
        loads.append(copy)

    barrier = pltpu.get_barrier_semaphore()
    for e in PARTNERS:
        pl.semaphore_signal(barrier, inc=1, device_id=member(*e), device_id_type=MESH)
    pl.semaphore_signal(barrier, inc=1, device_id=partner, device_id_type=MESH)

    lane = lax.broadcasted_iota(jnp.int32, (16, 128), 1)
    left = lane < 64
    action = lax.broadcasted_iota(jnp.int32, (16, 128), 0)
    for copy in small:
        copy.wait()
    for s in range(16):
        rows = pl.ds(s * 16, 16)
        masked[0, rows, :] = jnp.where(action < counts[s], costs[rows, :], jnp.float32(BIG))

    pl.semaphore_wait(barrier, len(PARTNERS) + 1)

    def to_partner(src, dst, k):
        copy = pltpu.make_async_remote_copy(
            src, dst, pair_send.at[k], pair_recv.at[k], device_id=partner, device_id_type=MESH
        )
        copy.start()
        return copy

    send_start = to_partner(start, swap.at[0], 0)
    send_cost = to_partner(masked.at[0], masked.at[1], 1)
    exchanges = []
    for i in range(4):
        rows = pl.ds(i * quarter, quarter)
        copy = pltpu.make_async_remote_copy(
            trans.at[rows],
            raw.at[1, rows],
            raw_send.at[i],
            raw_recv.at[i],
            device_id=partner,
            device_id_type=MESH,
        )
        copy.start()
        exchanges.append(copy)

    keep = jnp.logical_xor(left, c == 1)

    def both_halves(v):
        return jnp.where(keep[: v.shape[0]], v, pltpu.roll(v, 64, 1))

    send_start.wait_recv()
    left8 = lax.broadcasted_iota(jnp.int32, (8, 128), 1) < 64
    own = both_halves(start[...])
    other = both_halves(swap[0])
    own = jnp.where(left8, own[:8], own[8:])
    other = jnp.where(left8, other[:8], other[8:])
    values[0, here, 0:8, :] = jnp.where(c == 0, own, other)
    values[0, here, 8:16, :] = jnp.where(c == 0, other, own)

    def split_rows(which, base):
        def step(i, _):
            rows = pl.ds(pl.multiple_of(i * 16, 16), 16)
            out_rows = pl.ds(pl.multiple_of(base + i * 16, 16), 16)
            for g in range(32):
                v = raw[which, rows, g * 128 : (g + 1) * 128]
                h = v.astype(jnp.bfloat16)
                hi[g // ZS, g % ZS, out_rows, :] = h
                lo[g // ZS, g % ZS, out_rows, :] = (v - h.astype(jnp.float32)).astype(jnp.bfloat16)
            return 0

        lax.fori_loop(0, 16, step, 0)

    def receive_sem(t, d):
        if d in HOLDERS:
            return hold_recv.at[t, HOLDERS[d]]
        g0, g1 = group_of(d, 0), group_of(d, 1)
        return leaf_recv.at[t, g0 + c * (g1 - g0)]

    def hand_on(t, p, receivers):
        chunk = source(p)
        if p:
            wait_bytes(values.at[t, chunk], hold_recv.at[t, HOLDERS[p]])
        for d in receivers:
            pltpu.make_async_remote_copy(
                values.at[t, chunk],
                values.at[t, chunk],
                send_sem.at[t],
                receive_sem(t, d),
                device_id=member(*step(d, p)),
                device_id_type=MESH,
            ).start()

    def wait_bytes(ref, sem):
        pltpu.make_async_copy(ref, ref, sem).wait()

    def wait_group(t, i):
        for core in range(2):
            n = sum(group_of(d, core) == i for d in LEAVES)

            @pl.when(c == core)
            def _():
                if n:
                    wait_bytes(values.at[t, 0:n], leaf_recv.at[t, i])

    def multiply(t, i, base):
        blocks = []
        for (y0, z0), (y1, z1) in zip(GROUPS[0][i], GROUPS[1][i]):
            blocks.append((wrap(y + y0 + c * (y1 - y0), 4), wrap(z + z0 + c * (z1 - z0), ZS)))
        n = len(blocks)
        v = jnp.concatenate([values[t, pl.ds((k[0] * ZS + k[1]) * XS, XS)].reshape(64, 128) for k in blocks], axis=0) - base
        h = v.astype(jnp.bfloat16).astype(jnp.float32)
        r = v - h
        l_ = lax.broadcasted_iota(jnp.int32, v.shape, 1) < 64
        turned = pltpu.roll(jnp.where(l_, r, h), 64, 1)
        top = jnp.where(l_, h, turned).reshape(n * 8, 1, 8, 128)
        bottom = jnp.where(l_, turned, r).reshape(n * 8, 1, 8, 128)
        w = jnp.concatenate([top, bottom], axis=1).reshape(n * 128, 128).astype(jnp.bfloat16)
        rows = [half[k[0], k[1]] for half in (hi, lo) for k in blocks]
        part = jnp.dot(
            jnp.concatenate(rows, axis=1), jnp.concatenate([w, w], axis=0), preferred_element_type=jnp.float32
        )
        if i == 0:
            total[...] = part
        else:
            total[...] += part

    def finish_costs():
        send_cost.wait_recv()

        def step(i, _):
            for which in range(2):
                rows = pl.ds(pl.multiple_of(i * 16, 16), 16)
                base = (c if which == 0 else 1 - c) * 256
                cost2[pl.ds(pl.multiple_of(base + i * 16, 16), 16), :] = both_halves(masked[which, rows, :])
            return 0

        lax.fori_loop(0, 16, step, 0)

    mine[0] = jnp.full((8, 128), -BIG, jnp.float32)
    row8 = lax.broadcasted_iota(jnp.int32, (8, 128), 0)
    lane8 = lax.broadcasted_iota(jnp.int32, (8, 128), 1)

    def iteration(t, _):
        hand_on(t, *TREE[0])

        @pl.when(t == 0)
        def _():
            for copy in loads:
                copy.wait()
            split_rows(0, c * 256)

        for p, receivers in TREE[1:]:
            hand_on(t, p, receivers)

        @pl.when(t == 0)
        def _():
            finish_costs()
            for copy in exchanges:
                copy.wait_recv()
            split_rows(1, (1 - c) * 256)

        packed = values[t, here]
        base = packed[0:1, :]
        base = jnp.where(lax.broadcasted_iota(jnp.int32, (1, 128), 1) < 64, base, pltpu.roll(base, 64, 1))

        for i in range(len(GROUPS[0])):
            wait_group(t, i)
            multiply(t, i, base)

        e = total[...]
        q = e + pltpu.roll(e, 64, 1) + cost2[...]
        best = jnp.min(q.reshape(32, 16, 128), axis=1) + base
        best_io[0] = best[:16]
        best_io[1] = best[16:]
        new = jnp.concatenate(
            [jnp.where(left8, best[0:8], best[8:16]), jnp.where(left8, best[16:24], best[24:32])], axis=0
        )
        values[t + 1, here] = new
        inc = new - packed
        up = jnp.max(inc, axis=0, keepdims=True)
        down = jnp.max(-inc, axis=0, keepdims=True)
        up = jnp.maximum(up, pltpu.roll(up, 64, 1))
        down = jnp.maximum(down, pltpu.roll(down, 64, 1))
        mine[0] = jnp.where(row8 == t, jnp.where(lane8 < 64, up, down), mine[0])

        return 0

    lax.fori_loop(0, ITERS, iteration, 0)

    device = (y * ZS + z) * XS + x
    ids = device * 32 + lax.broadcasted_iota(jnp.int32, (16, 128), 0)
    picked = jnp.maximum(
        jnp.where(ids == ref_state[0], best_io[0], -BIG), jnp.where(ids + 16 == ref_state[0], best_io[1], -BIG)
    )
    ref_row = jnp.max(picked, axis=0, keepdims=True)
    mine[0] = jnp.where(row8 == 4, ref_row, mine[0])
    send_best = to_partner(best_io.at[1 - c], swap.at[1], 2)

    for da, dz in PLANE:
        pltpu.make_async_remote_copy(
            mine.at[0],
            plane_in.at[da * ZS + dz - 1],
            send_sem.at[4],
            plane_recv.at[da * ZS + dz - 1],
            device_id=member(da, dz, 0),
            device_id_type=MESH,
        ).start()
    top = mine[0]
    for da, dz in PLANE:
        pltpu.make_async_remote_copy(
            mine.at[0],
            plane_in.at[da * ZS + dz - 1],
            send_sem.at[4],
            plane_recv.at[da * ZS + dz - 1],
            device_id=partner,
            device_id_type=MESH,
        ).wait_recv()
        top = jnp.maximum(top, plane_in[da * ZS + dz - 1])
    mine[1] = top
    lines = []
    for db in (2, 1, 3):
        copy = pltpu.make_async_remote_copy(
            mine.at[1],
            line_in.at[db],
            line_send.at[0],
            line_recv.at[db],
            device_id=member(0, 0, db),
            device_id_type=MESH,
        )
        copy.start()
        lines.append((copy, db))
    for copy, db in lines:
        copy.wait_recv()
        top = jnp.maximum(top, line_in[db])
    half_in[0] = top
    send_half = to_partner(half_in.at[0], half_in.at[1], 3)
    send_half.wait_recv()
    other = half_in[1]
    r0 = jnp.where(c == 0, top, other)
    r1 = jnp.where(c == 0, other, top)
    upper = jnp.where(left8, r0, pltpu.roll(r1, 64, 1))
    lower = -jnp.where(left8, pltpu.roll(r0, 64, 1), r1)
    ref_full = jnp.where(left8, r0, r1)[4:5]
    out[16:20, :] = upper[0:4]
    out[20:24, :] = lower[0:4]
    send_best.wait_recv()
    out[0:16, :] = jnp.where(keep, jnp.where(c == 0, best_io[0], best_io[1]), swap[1]) - ref_full

    def sent(t, _):
        wait_bytes(values.at[t, 0:127], send_sem.at[t])
        return 0

    lax.fori_loop(0, ITERS, sent, 0)
    wait_bytes(plane_in.at[0:31], send_sem.at[4])
    part = line_in.at[0:3]
    pltpu.make_async_copy(part, part, line_send.at[0]).wait()
    for copy in (send_start, send_cost, send_best, send_half, *exchanges):
        copy.wait_send()


def deal(out, relative, lower, upper):
    relative[...] = out[0:16, :]
    upper[...] = out[16:20, :]
    lower[...] = out[20:24, :]


def local(transitions, costs, valid_counts, start_values, ref_state):
    dma = pltpu.SemaphoreType.DMA
    f32, bf16 = jnp.float32, jnp.bfloat16
    vmem = pl.BlockSpec(memory_space=pltpu.VMEM)
    out = pl.pallas_call(
        kernel,
        out_shape=jax.ShapeDtypeStruct((24, 128), f32),
        in_specs=[pl.BlockSpec(memory_space=pl.ANY)] * 5,
        out_specs=vmem,
        scratch_shapes=[
            pltpu.VMEM((ITERS + 1, YS * ZS * XS, 16, 128), f32),
            pltpu.VMEM((256, 128), f32),
            pltpu.SMEM((16,), jnp.int32),
            pltpu.VMEM((16, 128), f32),
            pltpu.SMEM((1,), jnp.int32),
            pltpu.VMEM((2, 256, 4096), f32),
            pltpu.VMEM((YS, ZS, 512, 128), bf16),
            pltpu.VMEM((YS, ZS, 512, 128), bf16),
            pltpu.VMEM((2, 256, 128), f32),
            pltpu.VMEM((512, 128), f32),
            pltpu.VMEM((512, 128), f32),
            pltpu.VMEM((2, 16, 128), f32),
            pltpu.VMEM((2, 8, 128), f32),
            pltpu.VMEM((4 * ZS - 1, 8, 128), f32),
            pltpu.VMEM((4, 8, 128), f32),
            pltpu.VMEM((2, 8, 128), f32),
            pltpu.VMEM((2, 16, 128), f32),
            dma((ITERS, len(TREE))),
            dma((ITERS, len(GROUPS[0]))),
            dma((4 * ZS - 1,)),
            dma((4,)),
            dma((ITERS + 1,)),
            dma((1,)),
            dma((4,)),
            dma((4,)),
            dma((4,)),
            dma((4,)),
            dma((4,)),
            dma((4,)),
        ],
        compiler_params=pltpu.CompilerParams(
            collective_id=0, has_side_effects=True, vmem_limit_bytes=60 * 1024 * 1024
        ),
        name="value_iteration",
    )(
        transitions.reshape(256, 4096),
        costs.reshape(256, 128),
        valid_counts,
        start_values,
        ref_state,
    )
    return pl.pallas_call(
        deal,
        out_shape=(
            jax.ShapeDtypeStruct((16, 128), f32),
            jax.ShapeDtypeStruct((ITERS, 128), f32),
            jax.ShapeDtypeStruct((ITERS, 128), f32),
        ),
        in_specs=[vmem],
        out_specs=(vmem, vmem, vmem),
        name="deal",
    )(out)


def solution(mesh):
    split = Mesh(mesh.devices.reshape(YS, ZS, XS, 2), AXES)
    return jax.shard_map(
        local,
        mesh=split,
        in_specs=(P(AXES, None, None), P(AXES, None, None), P(AXES), P(AXES, None), P()),
        out_specs=(P(AXES, None), P(), P()),
        check_vma=False,
    )
```

```python
import functools

import jax
import jax.numpy as jnp
from jax import lax
from jax.experimental import pallas as pl
from jax.experimental.pallas import tpu as pltpu
from jax.sharding import Mesh
from jax.sharding import PartitionSpec as P

ITERS = 4
YS, ZS, XS = 4, 8, 4
AXES = ("y", "z", "x", "c")
BIG = 1e30
MESH = pl.DeviceIdType.MESH


def ring(delta, size):
    return min(delta, size - delta)


PLANE = sorted(
    ((da, dz) for da in range(4) for dz in range(ZS) if da or dz),
    key=lambda d: (ring(d[0], 4) + ring(d[1], ZS), ring(d[1], ZS), d),
)

TREE = (
    (0, (31, 32, 12, 25, 21, 20, 7, 4, 19, 91, 99, 105, 89, 34, 58, 28, 35, 40, 1, 96, 72, 125, 92, 107, 42, 3, 70, 100, 98, 2, 127)),
    (32, (64, 67, 63, 37, 65)),
    (4, (9, 38, 36, 69, 5, 102)),
    (28, (29, 60, 124)),
    (96, (97,)),
    (31, (26, 27, 95, 126, 30)),
    (7, (71, 10, 39, 6, 103, 11)),
    (1, (33,)),
    (99, (111,)),
    (12, (14, 44, 8, 15, 108, 13)),
    (100, (68,)),
    (20, (120, 24, 23, 56, 119, 55, 116, 16, 52)),
    (40, (41, 43)),
    (92, (88, 84)),
    (105, (109, 73, 106, 101, 110, 104, 113, 74)),
    (34, (66, 62, 94)),
    (21, (22, 117, 53, 54, 17, 118)),
    (72, (75, 77, 76)),
    (91, (79, 90, 59, 87, 123, 86, 80)),
    (89, (93, 85, 122, 81, 121, 57)),
    (19, (18, 112, 115, 51, 82, 49, 114, 48, 83)),
    (42, (78, 50, 47, 46)),
    (60, (61,)),
    (44, (45,)),
)
GROUPS = (
    (
        ((0, 0), (0, 1), (1, 0), (0, 7), (3, 0), (1, 1), (0, 6), (3, 7), (0, 2), (2, 7), (0, 5), (3, 6)),
        ((2, 0), (1, 7), (0, 3), (1, 6), (2, 2), (2, 6), (3, 2), (3, 3), (1, 5), (1, 3), (0, 4), (2, 1)),
        ((2, 3), (3, 1), (1, 2), (1, 4)),
        ((2, 4), (3, 4), (2, 5), (3, 5)),
    ),
    (
        ((0, 0), (0, 1), (1, 0), (3, 0), (1, 1), (0, 7), (1, 7), (2, 7), (2, 0), (3, 7), (0, 6), (3, 6)),
        ((1, 6), (0, 2), (0, 3), (0, 5), (1, 2), (1, 3), (2, 6), (2, 1), (3, 3), (3, 2), (2, 3), (3, 1)),
        ((2, 2), (1, 4), (2, 4), (0, 4)),
        ((1, 5), (3, 4), (2, 5), (3, 5)),
    ),
)


def parts(d):
    return d // 32, d // 4 % ZS, d % 4


def step(d, p):
    return tuple((i - j) % n for i, j, n in zip(parts(d), parts(p), (4, ZS, 4)))


HOLDERS = {p: i for i, (p, _) in enumerate(TREE)}
LINE = ((0, 0, 2), (0, 0, 1), (0, 0, 3))
PARTNERS = sorted(
    {step(d, p) for p, receivers in TREE for d in receivers} | {(da, dz, 0) for da, dz in PLANE} | set(LINE)
)
PARTNERS = sorted(set(PARTNERS) | {tuple(-i % n for i, n in zip(e, (4, ZS, 4))) for e in PARTNERS})


def group_of(d, c):
    a, z, b = step(0, d)
    block = (a if c == 0 else b, z)
    return next(i for i, g in enumerate(GROUPS[c]) if block in g)


LEAVES = [d for d in range(1, 128) if d not in HOLDERS]


def kernel(
    trans,
    costs_in,
    counts_in,
    start_in,
    ref_in,
    out,
    values,
    costs,
    counts,
    start,
    ref_state,
    raw,
    hi,
    lo,
    masked,
    cost2,
    total,
    swap,
    mine,
    plane_in,
    line_in,
    bounds,
    best_io,
    hold_recv,
    leaf_recv,
    plane_recv,
    line_recv,
    send_sem,
    line_send,
    small_sem,
    raw_sem,
    raw_send,
    raw_recv,
    pair_send,
    pair_recv,
):
    y, z, x, c = (lax.axis_index(a) for a in AXES)
    a = y + c * (x - y)
    b = x + c * (y - x)

    def wrap(i, size):
        return lax.rem(i + size, size)

    def place(a_, z_, b_):
        y_ = a_ + c * (b_ - a_)
        x_ = b_ + c * (a_ - b_)
        return y_, z_, x_

    partner = (y, z, x, 1 - c)
    here = (y * ZS + z) * XS + x

    def member(da, dz, db):
        return (*place(wrap(a + da, 4), wrap(z + dz, ZS), wrap(b + db, 4)), c)

    def other_core(da, dz, db):
        return (*place(wrap(a + da, 4), wrap(z + dz, ZS), wrap(b + db, 4)), 1 - c)

    def source(d):
        da, dz, db = parts(d)
        y_, z_, x_ = place(wrap(a - da, 4), wrap(z - dz, ZS), wrap(b - db, 4))
        return (y_ * ZS + z_) * XS + x_

    small = []
    for i, (src, dst) in enumerate(
        ((start_in, start), (costs_in, costs), (counts_in, counts), (ref_in, ref_state))
    ):
        copy = pltpu.make_async_copy(src, dst, small_sem.at[i])
        copy.start()
        small.append(copy)
    quarter = 64
    loads = []
    for i in range(4):
        rows = pl.ds(i * quarter, quarter)
        copy = pltpu.make_async_copy(trans.at[rows], raw.at[0, rows], raw_sem.at[i])
        copy.start()
        loads.append(copy)

    barrier = pltpu.get_barrier_semaphore()
    for e in PARTNERS:
        pl.semaphore_signal(barrier, inc=1, device_id=member(*e), device_id_type=MESH)
    pl.semaphore_signal(barrier, inc=1, device_id=partner, device_id_type=MESH)
    for e in LINE:
        pl.semaphore_signal(barrier, inc=1, device_id=other_core(*e), device_id_type=MESH)
        pl.semaphore_signal(barrier, inc=1, device_id=other_core(*e[::-1]), device_id_type=MESH)

    lane = lax.broadcasted_iota(jnp.int32, (16, 128), 1)
    left = lane < 64
    action = lax.broadcasted_iota(jnp.int32, (16, 128), 0)
    for copy in small:
        copy.wait()
    for s in range(16):
        rows = pl.ds(s * 16, 16)
        masked[0, rows, :] = jnp.where(action < counts[s], costs[rows, :], jnp.float32(BIG))

    pl.semaphore_wait(barrier, len(PARTNERS) + 1 + 2 * len(LINE))

    def to_partner(src, dst, k):
        copy = pltpu.make_async_remote_copy(
            src, dst, pair_send.at[k], pair_recv.at[k], device_id=partner, device_id_type=MESH
        )
        copy.start()
        return copy

    send_start = to_partner(start, swap.at[0], 0)
    send_cost = to_partner(masked.at[0], masked.at[1], 1)
    exchanges = []
    for i in range(4):
        rows = pl.ds(i * quarter, quarter)
        copy = pltpu.make_async_remote_copy(
            trans.at[rows],
            raw.at[1, rows],
            raw_send.at[i],
            raw_recv.at[i],
            device_id=partner,
            device_id_type=MESH,
        )
        copy.start()
        exchanges.append(copy)

    keep = jnp.logical_xor(left, c == 1)

    def both_halves(v):
        return jnp.where(keep[: v.shape[0]], v, pltpu.roll(v, 64, 1))

    send_start.wait_recv()
    left8 = lax.broadcasted_iota(jnp.int32, (8, 128), 1) < 64
    own = both_halves(start[...])
    other = both_halves(swap[0])
    own = jnp.where(left8, own[:8], own[8:])
    other = jnp.where(left8, other[:8], other[8:])
    values[0, here, 0:8, :] = jnp.where(c == 0, own, other)
    values[0, here, 8:16, :] = jnp.where(c == 0, other, own)

    def split_rows(which, base):
        def step(i, _):
            rows = pl.ds(pl.multiple_of(i * 16, 16), 16)
            out_rows = pl.ds(pl.multiple_of(base + i * 16, 16), 16)
            for g in range(32):
                v = raw[which, rows, g * 128 : (g + 1) * 128]
                h = v.astype(jnp.bfloat16)
                hi[g // ZS, g % ZS, out_rows, :] = h
                lo[g // ZS, g % ZS, out_rows, :] = (v - h.astype(jnp.float32)).astype(jnp.bfloat16)
            return 0

        lax.fori_loop(0, 16, step, 0)

    def receive_sem(t, d):
        if d in HOLDERS:
            return hold_recv.at[t, HOLDERS[d]]
        g0, g1 = group_of(d, 0), group_of(d, 1)
        return leaf_recv.at[t, g0 + c * (g1 - g0)]

    def hand_on(t, p, receivers):
        chunk = source(p)
        if p:
            wait_bytes(values.at[t, chunk], hold_recv.at[t, HOLDERS[p]])
        for d in receivers:
            pltpu.make_async_remote_copy(
                values.at[t, chunk],
                values.at[t, chunk],
                send_sem.at[t],
                receive_sem(t, d),
                device_id=member(*step(d, p)),
                device_id_type=MESH,
            ).start()

    def wait_bytes(ref, sem):
        pltpu.make_async_copy(ref, ref, sem).wait()

    def wait_group(t, i):
        for core in range(2):
            n = sum(group_of(d, core) == i for d in LEAVES)

            @pl.when(c == core)
            def _():
                if n:
                    wait_bytes(values.at[t, 0:n], leaf_recv.at[t, i])

    def multiply(t, i, base):
        blocks = []
        for (y0, z0), (y1, z1) in zip(GROUPS[0][i], GROUPS[1][i]):
            blocks.append((wrap(y + y0 + c * (y1 - y0), 4), wrap(z + z0 + c * (z1 - z0), ZS)))
        n = len(blocks)
        v = jnp.concatenate([values[t, pl.ds((k[0] * ZS + k[1]) * XS, XS)].reshape(64, 128) for k in blocks], axis=0) - base
        h = v.astype(jnp.bfloat16).astype(jnp.float32)
        r = v - h
        l_ = lax.broadcasted_iota(jnp.int32, v.shape, 1) < 64
        turned = pltpu.roll(jnp.where(l_, r, h), 64, 1)
        top = jnp.where(l_, h, turned).reshape(n * 8, 1, 8, 128)
        bottom = jnp.where(l_, turned, r).reshape(n * 8, 1, 8, 128)
        w = jnp.concatenate([top, bottom], axis=1).reshape(n * 128, 128).astype(jnp.bfloat16)
        rows = [half[k[0], k[1]] for half in (hi, lo) for k in blocks]
        part = jnp.dot(
            jnp.concatenate(rows, axis=1), jnp.concatenate([w, w], axis=0), preferred_element_type=jnp.float32
        )
        if i == 0:
            total[...] = part
        else:
            total[...] += part

    def finish_costs():
        send_cost.wait_recv()

        def step(i, _):
            for which in range(2):
                rows = pl.ds(pl.multiple_of(i * 16, 16), 16)
                base = (c if which == 0 else 1 - c) * 256
                cost2[pl.ds(pl.multiple_of(base + i * 16, 16), 16), :] = both_halves(masked[which, rows, :])
            return 0

        lax.fori_loop(0, 16, step, 0)

    row8 = lax.broadcasted_iota(jnp.int32, (8, 128), 0)
    lane8 = lax.broadcasted_iota(jnp.int32, (8, 128), 1)

    def iteration(t, _):
        hand_on(t, *TREE[0])

        @pl.when(t == 0)
        def _():
            for copy in loads:
                copy.wait()
            split_rows(0, c * 256)

        for p, receivers in TREE[1:]:
            hand_on(t, p, receivers)

        @pl.when(t == 0)
        def _():
            finish_costs()
            for copy in exchanges:
                copy.wait_recv()
            split_rows(1, (1 - c) * 256)

        packed = values[t, here]
        base = packed[0:1, :]
        base = jnp.where(lax.broadcasted_iota(jnp.int32, (1, 128), 1) < 64, base, pltpu.roll(base, 64, 1))

        for i in range(len(GROUPS[0])):
            wait_group(t, i)
            multiply(t, i, base)

        e = total[...]
        q = e + pltpu.roll(e, 64, 1) + cost2[...]
        best = jnp.min(q.reshape(32, 16, 128), axis=1) + base
        best_io[0] = best[:16]
        best_io[1] = best[16:]
        new = jnp.concatenate(
            [jnp.where(left8, best[0:8], best[8:16]), jnp.where(left8, best[16:24], best[24:32])], axis=0
        )
        values[t + 1, here] = new
        return 0

    lax.fori_loop(0, ITERS, iteration, 0)

    device = (y * ZS + z) * XS + x
    ids = device * 32 + lax.broadcasted_iota(jnp.int32, (16, 128), 0)
    picked = jnp.maximum(
        jnp.where(ids == ref_state[0], best_io[0], -BIG), jnp.where(ids + 16 == ref_state[0], best_io[1], -BIG)
    )
    ref_row = jnp.max(picked, axis=0, keepdims=True)

    def bounds_of(inc):
        up = jnp.max(inc, axis=0, keepdims=True)
        down = jnp.max(-inc, axis=0, keepdims=True)
        up = jnp.maximum(up, pltpu.roll(up, 64, 1))
        down = jnp.maximum(down, pltpu.roll(down, 64, 1))
        return jnp.where(lane8[:1] < 64, up, down)

    mine[0] = jnp.concatenate([bounds_of(values[ITERS, here] - values[ITERS - 1, here]), ref_row], axis=0)
    send_best = to_partner(best_io.at[1 - c], swap.at[1], 2)

    for da, dz in PLANE:
        pltpu.make_async_remote_copy(
            mine.at[0],
            plane_in.at[da * ZS + dz - 1],
            send_sem.at[4],
            plane_recv.at[da * ZS + dz - 1],
            device_id=member(da, dz, 0),
            device_id_type=MESH,
        ).start()

    def increases(t, _):
        def block(i, carry):
            up, down = carry
            chunks = pl.ds(pl.multiple_of(i * 8, 8), 8)
            inc = values[t + 1, chunks] - values[t, chunks]
            inc = inc.reshape(16, 8, 128)
            return jnp.maximum(up, jnp.max(inc, axis=0)), jnp.maximum(down, jnp.max(-inc, axis=0))

        low = jnp.full((8, 128), -BIG, jnp.float32)
        up, down = lax.fori_loop(0, YS * ZS * XS // 8, block, (low, low))
        up = jnp.max(up, axis=0, keepdims=True)
        down = jnp.max(down, axis=0, keepdims=True)
        up = jnp.maximum(up, pltpu.roll(up, 64, 1))
        down = jnp.maximum(down, pltpu.roll(down, 64, 1))
        bounds[0] = jnp.where(row8 == t, jnp.where(lane8 < 64, up, down), bounds[0])
        return 0

    bounds[0] = jnp.full((8, 128), -BIG, jnp.float32)
    lax.fori_loop(0, ITERS - 1, increases, 0)
    send_bounds = to_partner(bounds.at[0], bounds.at[1], 3)
    top = mine[0]
    for da, dz in PLANE:
        pltpu.make_async_remote_copy(
            mine.at[0],
            plane_in.at[da * ZS + dz - 1],
            send_sem.at[4],
            plane_recv.at[da * ZS + dz - 1],
            device_id=partner,
            device_id_type=MESH,
        ).wait_recv()
        top = jnp.maximum(top, plane_in[da * ZS + dz - 1])
    mine[1] = top
    lines = []
    for db in (2, 1, 3):
        for k, device in enumerate((other_core(0, 0, db), member(0, 0, db))):
            copy = pltpu.make_async_remote_copy(
                mine.at[1],
                line_in.at[4 * k + db],
                line_send.at[4 * k + db],
                line_recv.at[4 * k + db],
                device_id=device,
                device_id_type=MESH,
            )
            copy.start()
            lines.append(copy)
    copy = pltpu.make_async_remote_copy(
        mine.at[1], line_in.at[0], line_send.at[0], line_recv.at[0], device_id=partner, device_id_type=MESH
    )
    copy.start()
    lines.append(copy)
    for copy in lines:
        copy.wait_recv()
    other = jnp.maximum(jnp.maximum(line_in[0], line_in[1]), jnp.maximum(line_in[2], line_in[3]))
    top = jnp.maximum(jnp.maximum(top, line_in[5]), jnp.maximum(line_in[6], line_in[7]))
    send_bounds.wait_recv()
    own_bounds = jnp.where(row8 == ITERS - 1, top[0:1], bounds[0])
    other_bounds = jnp.where(row8 == ITERS - 1, other[0:1], bounds[1])
    r0 = jnp.where(c == 0, own_bounds, other_bounds)
    r1 = jnp.where(c == 0, other_bounds, own_bounds)
    upper = jnp.where(left8, r0, pltpu.roll(r1, 64, 1))
    lower = -jnp.where(left8, pltpu.roll(r0, 64, 1), r1)
    ref_full = jnp.where(jnp.logical_xor(left8[:1], c == 1), top[1:2], other[1:2])
    out[16:20, :] = upper[0:4]
    out[20:24, :] = lower[0:4]
    send_best.wait_recv()
    out[0:16, :] = jnp.where(keep, jnp.where(c == 0, best_io[0], best_io[1]), swap[1]) - ref_full

    def sent(t, _):
        wait_bytes(values.at[t, 0:127], send_sem.at[t])
        return 0

    lax.fori_loop(0, ITERS, sent, 0)
    wait_bytes(plane_in.at[0:31], send_sem.at[4])
    for copy in (send_start, send_cost, send_best, send_bounds, *lines, *exchanges):
        copy.wait_send()


def deal(out, relative, lower, upper):
    relative[...] = out[0:16, :]
    upper[...] = out[16:20, :]
    lower[...] = out[20:24, :]


def local(transitions, costs, valid_counts, start_values, ref_state):
    dma = pltpu.SemaphoreType.DMA
    f32, bf16 = jnp.float32, jnp.bfloat16
    vmem = pl.BlockSpec(memory_space=pltpu.VMEM)
    out = pl.pallas_call(
        kernel,
        out_shape=jax.ShapeDtypeStruct((24, 128), f32),
        in_specs=[pl.BlockSpec(memory_space=pl.ANY)] * 5,
        out_specs=vmem,
        scratch_shapes=[
            pltpu.VMEM((ITERS + 1, YS * ZS * XS, 16, 128), f32),
            pltpu.VMEM((256, 128), f32),
            pltpu.SMEM((16,), jnp.int32),
            pltpu.VMEM((16, 128), f32),
            pltpu.SMEM((1,), jnp.int32),
            pltpu.VMEM((2, 256, 4096), f32),
            pltpu.VMEM((YS, ZS, 512, 128), bf16),
            pltpu.VMEM((YS, ZS, 512, 128), bf16),
            pltpu.VMEM((2, 256, 128), f32),
            pltpu.VMEM((512, 128), f32),
            pltpu.VMEM((512, 128), f32),
            pltpu.VMEM((2, 16, 128), f32),
            pltpu.VMEM((2, 2, 128), f32),
            pltpu.VMEM((4 * ZS - 1, 2, 128), f32),
            pltpu.VMEM((8, 2, 128), f32),
            pltpu.VMEM((2, 8, 128), f32),
            pltpu.VMEM((2, 16, 128), f32),
            dma((ITERS, len(TREE))),
            dma((ITERS, len(GROUPS[0]))),
            dma((4 * ZS - 1,)),
            dma((8,)),
            dma((ITERS + 1,)),
            dma((8,)),
            dma((4,)),
            dma((4,)),
            dma((4,)),
            dma((4,)),
            dma((4,)),
            dma((4,)),
        ],
        compiler_params=pltpu.CompilerParams(
            collective_id=0, has_side_effects=True, vmem_limit_bytes=60 * 1024 * 1024
        ),
        name="value_iteration",
    )(
        transitions.reshape(256, 4096),
        costs.reshape(256, 128),
        valid_counts,
        start_values,
        ref_state,
    )
    return pl.pallas_call(
        deal,
        out_shape=(
            jax.ShapeDtypeStruct((16, 128), f32),
            jax.ShapeDtypeStruct((ITERS, 128), f32),
            jax.ShapeDtypeStruct((ITERS, 128), f32),
        ),
        in_specs=[vmem],
        out_specs=(vmem, vmem, vmem),
        name="deal",
    )(out)


def solution(mesh):
    split = Mesh(mesh.devices.reshape(YS, ZS, XS, 2), AXES)
    return jax.shard_map(
        local,
        mesh=split,
        in_specs=(P(AXES, None, None), P(AXES, None, None), P(AXES), P(AXES, None), P()),
        out_specs=(P(AXES, None), P(), P()),
        check_vma=False,
    )
```

```python
import functools

import jax
import jax.numpy as jnp
from jax import lax
from jax.experimental import pallas as pl
from jax.experimental.pallas import tpu as pltpu
from jax.sharding import Mesh
from jax.sharding import PartitionSpec as P

ITERS = 4
YS, ZS, XS = 4, 8, 4
AXES = ("y", "z", "x", "c")
BIG = 1e30
MESH = pl.DeviceIdType.MESH


def ring(delta, size):
    return min(delta, size - delta)


PLANE = sorted(
    ((da, dz) for da in range(4) for dz in range(ZS) if da or dz),
    key=lambda d: (ring(d[0], 4) + ring(d[1], ZS), ring(d[1], ZS), d),
)

TREE = (
    (0, (7, 20, 89, 4, 12, 31, 55, 70, 36, 8, 32, 27, 28, 64, 2, 91, 41, 117, 68, 88, 99, 97, 105, 35, 1, 98, 125, 38, 96, 44, 66, 127, 3, 112, 34, 33)),
    (4, (10, 37, 15, 100, 103, 5)),
    (32, (65, 60, 92, 67, 61)),
    (28, (120, 124, 29)),
    (7, (14, 39, 6, 11, 107)),
    (31, (62, 30, 63)),
    (20, (21, 25, 53, 118, 52, 24, 116, 23)),
    (8, (9,)),
    (12, (13,)),
    (27, (22, 122, 59, 56, 26, 58, 18, 123, 119)),
    (99, (95, 102)),
    (68, (71, 72, 69, 104, 75)),
    (89, (90, 85, 84, 94, 57)),
    (41, (46, 73, 74, 40, 42, 49)),
    (44, (43, 76, 47, 45, 79)),
    (125, (121, 93, 126)),
    (55, (82, 50, 54, 19, 51, 86, 87)),
    (105, (101, 110, 109, 106, 77)),
    (112, (16, 111, 81, 48, 80, 17, 114, 83, 108, 115, 113)),
    (70, (78,)),
)
GROUPS = (
    (
        ((0, 0), (1, 0), (3, 0), (0, 7), (3, 7), (0, 1), (2, 0), (0, 6), (0, 2), (2, 2), (3, 1), (0, 5)),
        ((2, 7), (0, 3), (1, 2), (1, 1), (3, 5), (1, 6), (3, 2), (1, 7), (3, 3), (2, 1), (1, 3), (2, 6)),
        ((3, 6), (1, 4), (2, 3), (0, 4), (3, 4), (1, 5), (2, 5), (2, 4)),
    ),
    (
        ((0, 0), (0, 7), (3, 0), (0, 1), (1, 0), (2, 0), (1, 2), (1, 7), (3, 3), (0, 2), (3, 6), (2, 7)),
        ((3, 2), (2, 1), (0, 6), (2, 2), (3, 1), (3, 7), (1, 3), (1, 1), (2, 6), (0, 3), (0, 5), (1, 6)),
        ((3, 5), (3, 4), (2, 3), (1, 4), (0, 4), (1, 5), (2, 5), (2, 4)),
    ),
)


def parts(d):
    return d // 32, d // 4 % ZS, d % 4


def step(d, p):
    return tuple((i - j) % n for i, j, n in zip(parts(d), parts(p), (4, ZS, 4)))


HOLDERS = {p: i for i, (p, _) in enumerate(TREE)}
LINE = ((0, 0, 2), (0, 0, 1), (0, 0, 3))
PARTNERS = sorted(
    {step(d, p) for p, receivers in TREE for d in receivers} | {(da, dz, 0) for da, dz in PLANE} | set(LINE)
)
PARTNERS = sorted(
    set(PARTNERS) | {tuple(-i % n for i, n in zip(e, (4, ZS, 4))) for e in PARTNERS},
    key=lambda e: (-sum(ring(i, n) for i, n in zip(e, (4, ZS, 4))), e),
)


def group_of(d, c):
    a, z, b = step(0, d)
    block = (a if c == 0 else b, z)
    return next(i for i, g in enumerate(GROUPS[c]) if block in g)


LEAVES = [d for d in range(1, 128) if d not in HOLDERS]


def kernel(
    trans,
    costs_in,
    counts_in,
    start_in,
    ref_in,
    out,
    values,
    costs,
    counts,
    start,
    ref_state,
    raw,
    hi,
    lo,
    masked,
    cost2,
    total,
    swap,
    mine,
    plane_in,
    line_in,
    bounds,
    best_io,
    hold_recv,
    leaf_recv,
    plane_recv,
    line_recv,
    send_sem,
    line_send,
    small_sem,
    raw_sem,
    raw_send,
    raw_recv,
    pair_send,
    pair_recv,
):
    y, z, x, c = (lax.axis_index(a) for a in AXES)
    a = y + c * (x - y)
    b = x + c * (y - x)

    def wrap(i, size):
        return lax.rem(i + size, size)

    def place(a_, z_, b_):
        y_ = a_ + c * (b_ - a_)
        x_ = b_ + c * (a_ - b_)
        return y_, z_, x_

    partner = (y, z, x, 1 - c)
    here = (y * ZS + z) * XS + x

    def member(da, dz, db):
        return (*place(wrap(a + da, 4), wrap(z + dz, ZS), wrap(b + db, 4)), c)

    def other_core(da, dz, db):
        return (*place(wrap(a + da, 4), wrap(z + dz, ZS), wrap(b + db, 4)), 1 - c)

    def source(d):
        da, dz, db = parts(d)
        y_, z_, x_ = place(wrap(a - da, 4), wrap(z - dz, ZS), wrap(b - db, 4))
        return (y_ * ZS + z_) * XS + x_

    small = []
    for i, (src, dst) in enumerate(
        ((start_in, start), (costs_in, costs), (counts_in, counts), (ref_in, ref_state))
    ):
        copy = pltpu.make_async_copy(src, dst, small_sem.at[i])
        copy.start()
        small.append(copy)
    quarter = 64
    loads = []
    for i in range(4):
        rows = pl.ds(i * quarter, quarter)
        copy = pltpu.make_async_copy(trans.at[rows], raw.at[0, rows], raw_sem.at[i])
        copy.start()
        loads.append(copy)

    barrier = pltpu.get_barrier_semaphore()
    for e in PARTNERS:
        pl.semaphore_signal(barrier, inc=1, device_id=member(*e), device_id_type=MESH)
    pl.semaphore_signal(barrier, inc=1, device_id=partner, device_id_type=MESH)
    for e in LINE:
        pl.semaphore_signal(barrier, inc=1, device_id=other_core(*e), device_id_type=MESH)
        pl.semaphore_signal(barrier, inc=1, device_id=other_core(*e[::-1]), device_id_type=MESH)

    lane = lax.broadcasted_iota(jnp.int32, (16, 128), 1)
    left = lane < 64
    action = lax.broadcasted_iota(jnp.int32, (16, 128), 0)
    for copy in small:
        copy.wait()
    for s in range(16):
        rows = pl.ds(s * 16, 16)
        masked[0, rows, :] = jnp.where(action < counts[s], costs[rows, :], jnp.float32(BIG))

    pl.semaphore_wait(barrier, len(PARTNERS) + 1 + 2 * len(LINE))

    def to_partner(src, dst, k):
        copy = pltpu.make_async_remote_copy(
            src, dst, pair_send.at[k], pair_recv.at[k], device_id=partner, device_id_type=MESH
        )
        copy.start()
        return copy

    send_start = to_partner(start, swap.at[0], 0)
    send_cost = to_partner(masked.at[0], masked.at[1], 1)
    exchanges = []
    for i in range(4):
        rows = pl.ds(i * quarter, quarter)
        copy = pltpu.make_async_remote_copy(
            trans.at[rows],
            raw.at[1, rows],
            raw_send.at[i],
            raw_recv.at[i],
            device_id=partner,
            device_id_type=MESH,
        )
        copy.start()
        exchanges.append(copy)

    keep = jnp.logical_xor(left, c == 1)

    def both_halves(v):
        return jnp.where(keep[: v.shape[0]], v, pltpu.roll(v, 64, 1))

    send_start.wait_recv()
    left8 = lax.broadcasted_iota(jnp.int32, (8, 128), 1) < 64
    own = both_halves(start[...])
    other = both_halves(swap[0])
    own = jnp.where(left8, own[:8], own[8:])
    other = jnp.where(left8, other[:8], other[8:])
    values[0, here, 0:8, :] = jnp.where(c == 0, own, other)
    values[0, here, 8:16, :] = jnp.where(c == 0, other, own)

    def split_rows(which, base):
        def step(i, _):
            rows = pl.ds(pl.multiple_of(i * 16, 16), 16)
            out_rows = pl.ds(pl.multiple_of(base + i * 16, 16), 16)
            for g in range(32):
                v = raw[which, rows, g * 128 : (g + 1) * 128]
                h = v.astype(jnp.bfloat16)
                hi[g // ZS, g % ZS, out_rows, :] = h
                lo[g // ZS, g % ZS, out_rows, :] = (v - h.astype(jnp.float32)).astype(jnp.bfloat16)
            return 0

        lax.fori_loop(0, 16, step, 0)

    def receive_sem(t, d):
        if d in HOLDERS:
            return hold_recv.at[t, HOLDERS[d]]
        g0, g1 = group_of(d, 0), group_of(d, 1)
        return leaf_recv.at[t, g0 + c * (g1 - g0)]

    def hand_on(t, p, receivers):
        chunk = source(p)
        if p:
            wait_bytes(values.at[t, chunk], hold_recv.at[t, HOLDERS[p]])
        for d in receivers:
            pltpu.make_async_remote_copy(
                values.at[t, chunk],
                values.at[t, chunk],
                send_sem.at[t],
                receive_sem(t, d),
                device_id=member(*step(d, p)),
                device_id_type=MESH,
            ).start()

    def wait_bytes(ref, sem):
        pltpu.make_async_copy(ref, ref, sem).wait()

    def wait_group(t, i):
        for core in range(2):
            n = sum(group_of(d, core) == i for d in LEAVES)

            @pl.when(c == core)
            def _():
                if n:
                    wait_bytes(values.at[t, 0:n], leaf_recv.at[t, i])

    def multiply(t, i, base):
        blocks = []
        for (y0, z0), (y1, z1) in zip(GROUPS[0][i], GROUPS[1][i]):
            blocks.append((wrap(y + y0 + c * (y1 - y0), 4), wrap(z + z0 + c * (z1 - z0), ZS)))
        n = len(blocks)
        v = jnp.concatenate([values[t, pl.ds((k[0] * ZS + k[1]) * XS, XS)].reshape(64, 128) for k in blocks], axis=0) - base
        h = v.astype(jnp.bfloat16).astype(jnp.float32)
        r = v - h
        l_ = lax.broadcasted_iota(jnp.int32, v.shape, 1) < 64
        turned = pltpu.roll(jnp.where(l_, r, h), 64, 1)
        top = jnp.where(l_, h, turned).reshape(n * 8, 1, 8, 128)
        bottom = jnp.where(l_, turned, r).reshape(n * 8, 1, 8, 128)
        w = jnp.concatenate([top, bottom], axis=1).reshape(n * 128, 128).astype(jnp.bfloat16)
        rows = [half[k[0], k[1]] for half in (hi, lo) for k in blocks]
        part = jnp.dot(
            jnp.concatenate(rows, axis=1), jnp.concatenate([w, w], axis=0), preferred_element_type=jnp.float32
        )
        if i == 0:
            total[...] = part
        else:
            total[...] += part

    def finish_costs():
        send_cost.wait_recv()

        def step(i, _):
            for which in range(2):
                rows = pl.ds(pl.multiple_of(i * 16, 16), 16)
                base = (c if which == 0 else 1 - c) * 256
                cost2[pl.ds(pl.multiple_of(base + i * 16, 16), 16), :] = both_halves(masked[which, rows, :])
            return 0

        lax.fori_loop(0, 16, step, 0)

    row8 = lax.broadcasted_iota(jnp.int32, (8, 128), 0)
    lane8 = lax.broadcasted_iota(jnp.int32, (8, 128), 1)

    def iteration(t, _):
        hand_on(t, *TREE[0])

        @pl.when(t == 0)
        def _():
            for copy in loads:
                copy.wait()
            split_rows(0, c * 256)

        for p, receivers in TREE[1:]:
            hand_on(t, p, receivers)

        @pl.when(t == 0)
        def _():
            finish_costs()
            for copy in exchanges:
                copy.wait_recv()
            split_rows(1, (1 - c) * 256)

        packed = values[t, here]
        base = packed[0:1, :]
        base = jnp.where(lax.broadcasted_iota(jnp.int32, (1, 128), 1) < 64, base, pltpu.roll(base, 64, 1))

        for i in range(len(GROUPS[0])):
            wait_group(t, i)
            multiply(t, i, base)

        e = total[...]
        q = e + pltpu.roll(e, 64, 1) + cost2[...]
        best = jnp.min(q.reshape(32, 16, 128), axis=1) + base
        best_io[0] = best[:16]
        best_io[1] = best[16:]
        new = jnp.concatenate(
            [jnp.where(left8, best[0:8], best[8:16]), jnp.where(left8, best[16:24], best[24:32])], axis=0
        )
        values[t + 1, here] = new
        return 0

    lax.fori_loop(0, ITERS, iteration, 0)

    device = (y * ZS + z) * XS + x
    ids = device * 32 + lax.broadcasted_iota(jnp.int32, (16, 128), 0)
    picked = jnp.maximum(
        jnp.where(ids == ref_state[0], best_io[0], -BIG), jnp.where(ids + 16 == ref_state[0], best_io[1], -BIG)
    )
    ref_row = jnp.max(picked, axis=0, keepdims=True)

    def bounds_of(inc):
        up = jnp.max(inc, axis=0, keepdims=True)
        down = jnp.max(-inc, axis=0, keepdims=True)
        up = jnp.maximum(up, pltpu.roll(up, 64, 1))
        down = jnp.maximum(down, pltpu.roll(down, 64, 1))
        return jnp.where(lane8[:1] < 64, up, down)

    mine[0] = jnp.concatenate([bounds_of(values[ITERS, here] - values[ITERS - 1, here]), ref_row], axis=0)
    send_best = to_partner(best_io.at[1 - c], swap.at[1], 2)

    for da, dz in PLANE[::-1]:
        pltpu.make_async_remote_copy(
            mine.at[0],
            plane_in.at[da * ZS + dz - 1],
            send_sem.at[4],
            plane_recv.at[da * ZS + dz - 1],
            device_id=member(da, dz, 0),
            device_id_type=MESH,
        ).start()

    def increases(t, _):
        def block(i, carry):
            up, down = carry
            chunks = pl.ds(pl.multiple_of(i * 8, 8), 8)
            inc = values[t + 1, chunks] - values[t, chunks]
            inc = inc.reshape(16, 8, 128)
            return jnp.maximum(up, jnp.max(inc, axis=0)), jnp.maximum(down, jnp.max(-inc, axis=0))

        low = jnp.full((8, 128), -BIG, jnp.float32)
        up, down = lax.fori_loop(0, YS * ZS * XS // 8, block, (low, low))
        up = jnp.max(up, axis=0, keepdims=True)
        down = jnp.max(down, axis=0, keepdims=True)
        up = jnp.maximum(up, pltpu.roll(up, 64, 1))
        down = jnp.maximum(down, pltpu.roll(down, 64, 1))
        bounds[0] = jnp.where(row8 == t, jnp.where(lane8 < 64, up, down), bounds[0])
        return 0

    bounds[0] = jnp.full((8, 128), -BIG, jnp.float32)
    lax.fori_loop(0, ITERS - 1, increases, 0)
    send_bounds = to_partner(bounds.at[0], bounds.at[1], 3)
    top = mine[0]
    for da, dz in PLANE:
        pltpu.make_async_remote_copy(
            mine.at[0],
            plane_in.at[da * ZS + dz - 1],
            send_sem.at[4],
            plane_recv.at[da * ZS + dz - 1],
            device_id=partner,
            device_id_type=MESH,
        ).wait_recv()
        top = jnp.maximum(top, plane_in[da * ZS + dz - 1])
    mine[1] = top
    lines = []
    for db in (2, 1, 3):
        for k, device in enumerate((other_core(0, 0, db), member(0, 0, db))):
            copy = pltpu.make_async_remote_copy(
                mine.at[1],
                line_in.at[4 * k + db],
                line_send.at[4 * k + db],
                line_recv.at[4 * k + db],
                device_id=device,
                device_id_type=MESH,
            )
            copy.start()
            lines.append(copy)
    copy = pltpu.make_async_remote_copy(
        mine.at[1], line_in.at[0], line_send.at[0], line_recv.at[0], device_id=partner, device_id_type=MESH
    )
    copy.start()
    lines.append(copy)
    for copy in lines:
        copy.wait_recv()
    other = jnp.maximum(jnp.maximum(line_in[0], line_in[1]), jnp.maximum(line_in[2], line_in[3]))
    top = jnp.maximum(jnp.maximum(top, line_in[5]), jnp.maximum(line_in[6], line_in[7]))
    send_bounds.wait_recv()
    own_bounds = jnp.where(row8 == ITERS - 1, top[0:1], bounds[0])
    other_bounds = jnp.where(row8 == ITERS - 1, other[0:1], bounds[1])
    r0 = jnp.where(c == 0, own_bounds, other_bounds)
    r1 = jnp.where(c == 0, other_bounds, own_bounds)
    upper = jnp.where(left8, r0, pltpu.roll(r1, 64, 1))
    lower = -jnp.where(left8, pltpu.roll(r0, 64, 1), r1)
    ref_full = jnp.where(jnp.logical_xor(left8[:1], c == 1), top[1:2], other[1:2])
    out[16:20, :] = upper[0:4]
    out[20:24, :] = lower[0:4]
    send_best.wait_recv()
    out[0:16, :] = jnp.where(keep, jnp.where(c == 0, best_io[0], best_io[1]), swap[1]) - ref_full

    def sent(t, _):
        wait_bytes(values.at[t, 0:127], send_sem.at[t])
        return 0

    lax.fori_loop(0, ITERS, sent, 0)
    wait_bytes(plane_in.at[0:31], send_sem.at[4])
    for copy in (send_start, send_cost, send_best, send_bounds, *lines, *exchanges):
        copy.wait_send()


def deal(out, relative, lower, upper):
    relative[...] = out[0:16, :]
    upper[...] = out[16:20, :]
    lower[...] = out[20:24, :]


def local(transitions, costs, valid_counts, start_values, ref_state):
    dma = pltpu.SemaphoreType.DMA
    f32, bf16 = jnp.float32, jnp.bfloat16
    vmem = pl.BlockSpec(memory_space=pltpu.VMEM)
    out = pl.pallas_call(
        kernel,
        out_shape=jax.ShapeDtypeStruct((24, 128), f32),
        in_specs=[pl.BlockSpec(memory_space=pl.ANY)] * 5,
        out_specs=vmem,
        scratch_shapes=[
            pltpu.VMEM((ITERS + 1, YS * ZS * XS, 16, 128), f32),
            pltpu.VMEM((256, 128), f32),
            pltpu.SMEM((16,), jnp.int32),
            pltpu.VMEM((16, 128), f32),
            pltpu.SMEM((1,), jnp.int32),
            pltpu.VMEM((2, 256, 4096), f32),
            pltpu.VMEM((YS, ZS, 512, 128), bf16),
            pltpu.VMEM((YS, ZS, 512, 128), bf16),
            pltpu.VMEM((2, 256, 128), f32),
            pltpu.VMEM((512, 128), f32),
            pltpu.VMEM((512, 128), f32),
            pltpu.VMEM((2, 16, 128), f32),
            pltpu.VMEM((2, 2, 128), f32),
            pltpu.VMEM((4 * ZS - 1, 2, 128), f32),
            pltpu.VMEM((8, 2, 128), f32),
            pltpu.VMEM((2, 8, 128), f32),
            pltpu.VMEM((2, 16, 128), f32),
            dma((ITERS, len(TREE))),
            dma((ITERS, len(GROUPS[0]))),
            dma((4 * ZS - 1,)),
            dma((8,)),
            dma((ITERS + 1,)),
            dma((8,)),
            dma((4,)),
            dma((4,)),
            dma((4,)),
            dma((4,)),
            dma((4,)),
            dma((4,)),
        ],
        compiler_params=pltpu.CompilerParams(
            collective_id=0, has_side_effects=True, vmem_limit_bytes=60 * 1024 * 1024
        ),
        name="value_iteration",
    )(
        transitions.reshape(256, 4096),
        costs.reshape(256, 128),
        valid_counts,
        start_values,
        ref_state,
    )
    return pl.pallas_call(
        deal,
        out_shape=(
            jax.ShapeDtypeStruct((16, 128), f32),
            jax.ShapeDtypeStruct((ITERS, 128), f32),
            jax.ShapeDtypeStruct((ITERS, 128), f32),
        ),
        in_specs=[vmem],
        out_specs=(vmem, vmem, vmem),
        name="deal",
    )(out)


def solution(mesh):
    split = Mesh(mesh.devices.reshape(YS, ZS, XS, 2), AXES)
    return jax.shard_map(
        local,
        mesh=split,
        in_specs=(P(AXES, None, None), P(AXES, None, None), P(AXES), P(AXES, None), P()),
        out_specs=(P(AXES, None), P(), P()),
        check_vma=False,
    )
```

```python
import functools

import jax
import jax.numpy as jnp
from jax import lax
from jax.experimental import pallas as pl
from jax.experimental.pallas import tpu as pltpu
from jax.sharding import Mesh
from jax.sharding import PartitionSpec as P

ITERS = 4
YS, ZS, XS = 4, 8, 4
AXES = ("y", "z", "x", "c")
BIG = 1e30
MESH = pl.DeviceIdType.MESH


def ring(delta, size):
    return min(delta, size - delta)


PLANE = sorted(
    ((da, dz) for da in range(4) for dz in range(ZS) if da or dz),
    key=lambda d: (ring(d[0], 4) + ring(d[1], ZS), ring(d[1], ZS), d),
)

TREE = (
    (0, (11, 1, 28, 92, 4, 13, 94, 36, 20, 75, 25, 32, 33, 101, 79, 123, 16, 35, 10, 66, 99, 70, 116, 2, 96, 3, 22, 64, 125, 97, 37, 103, 68, 31)),
    (1, (34, 98, 30, 85, 65, 5)),
    (28, (127, 124, 29, 60, 61, 95, 56)),
    (4, (105, 69, 6, 100, 7, 102)),
    (32, (62,)),
    (96, (104, 67)),
    (36, (71, 40, 38)),
    (11, (106, 8, 111, 47, 15)),
    (33, (93,)),
    (20, (23, 24, 21)),
    (35, (63, 59, 39)),
    (25, (121, 26, 57, 58)),
    (13, (73, 81, 45, 110, 12, 49, 14, 113, 9, 44, 17, 46, 77, 109)),
    (116, (114, 118, 112, 120, 84, 115, 108, 117, 52)),
    (123, (90, 88, 119, 122, 27, 87, 91)),
    (75, (74, 43, 107, 72)),
    (125, (126, 89)),
    (37, (41,)),
    (10, (42,)),
    (79, (76, 83, 78, 80, 51, 82)),
    (22, (50, 86, 18, 54)),
    (56, (48, 55)),
    (15, (19,)),
    (21, (53,)),
)
GROUPS = (
    (
        ((0, 0), (3, 0), (0, 1), (1, 0), (0, 7), (2, 0), (0, 3), (2, 1), (3, 7), (0, 6)),
        ((2, 7), (3, 1), (1, 7), (3, 2), (0, 5), (0, 2), (1, 2), (1, 6), (1, 1), (1, 5), (3, 5), (2, 6), (1, 3), (3, 6)),
        ((2, 5), (1, 4), (2, 2), (2, 4), (2, 3), (0, 4), (3, 3), (3, 4)),
    ),
    (
        ((0, 0), (0, 1), (0, 7), (2, 0), (3, 0), (1, 0), (1, 1), (3, 1), (1, 7), (3, 7)),
        ((2, 7), (1, 5), (0, 6), (2, 1), (1, 2), (3, 5), (3, 4), (1, 6), (3, 6), (2, 6), (0, 5), (2, 5), (0, 2), (0, 3)),
        ((2, 2), (3, 2), (2, 3), (2, 4), (1, 3), (3, 3), (0, 4), (1, 4)),
    ),
)


def parts(d):
    return d // 32, d // 4 % ZS, d % 4


def step(d, p):
    return tuple((i - j) % n for i, j, n in zip(parts(d), parts(p), (4, ZS, 4)))


HOLDERS = {p: i for i, (p, _) in enumerate(TREE)}
LINE = ((0, 0, 2), (0, 0, 1), (0, 0, 3))
PARTNERS = sorted(
    {step(d, p) for p, receivers in TREE for d in receivers} | {(da, dz, 0) for da, dz in PLANE} | set(LINE)
)
PARTNERS = sorted(
    set(PARTNERS) | {tuple(-i % n for i, n in zip(e, (4, ZS, 4))) for e in PARTNERS},
    key=lambda e: (-sum(ring(i, n) for i, n in zip(e, (4, ZS, 4))), e),
)


def group_of(d, c):
    a, z, b = step(0, d)
    block = (a if c == 0 else b, z)
    return next(i for i, g in enumerate(GROUPS[c]) if block in g)


LEAVES = [d for d in range(1, 128) if d not in HOLDERS]


def kernel(
    trans,
    costs_in,
    counts_in,
    start_in,
    ref_in,
    out,
    values,
    costs,
    counts,
    start,
    ref_state,
    raw,
    hi,
    lo,
    masked,
    cost2,
    total,
    swap,
    mine,
    plane_in,
    line_in,
    bounds,
    best_io,
    hold_recv,
    leaf_recv,
    plane_recv,
    line_recv,
    send_sem,
    line_send,
    small_sem,
    raw_sem,
    raw_send,
    raw_recv,
    pair_send,
    pair_recv,
):
    y, z, x, c = (lax.axis_index(a) for a in AXES)
    a = y + c * (x - y)
    b = x + c * (y - x)

    def wrap(i, size):
        return lax.rem(i + size, size)

    def place(a_, z_, b_):
        y_ = a_ + c * (b_ - a_)
        x_ = b_ + c * (a_ - b_)
        return y_, z_, x_

    partner = (y, z, x, 1 - c)
    here = (y * ZS + z) * XS + x

    def member(da, dz, db):
        return (*place(wrap(a + da, 4), wrap(z + dz, ZS), wrap(b + db, 4)), c)

    def other_core(da, dz, db):
        return (*place(wrap(a + da, 4), wrap(z + dz, ZS), wrap(b + db, 4)), 1 - c)

    def source(d):
        da, dz, db = parts(d)
        y_, z_, x_ = place(wrap(a - da, 4), wrap(z - dz, ZS), wrap(b - db, 4))
        return (y_ * ZS + z_) * XS + x_

    small = []
    for i, (src, dst) in enumerate(
        ((start_in, start), (costs_in, costs), (counts_in, counts), (ref_in, ref_state))
    ):
        copy = pltpu.make_async_copy(src, dst, small_sem.at[i])
        copy.start()
        small.append(copy)
    quarter = 64
    loads = []
    for i in range(4):
        rows = pl.ds(i * quarter, quarter)
        copy = pltpu.make_async_copy(trans.at[rows], raw.at[0, rows], raw_sem.at[i])
        copy.start()
        loads.append(copy)

    barrier = pltpu.get_barrier_semaphore()
    for e in PARTNERS:
        pl.semaphore_signal(barrier, inc=1, device_id=member(*e), device_id_type=MESH)
    pl.semaphore_signal(barrier, inc=1, device_id=partner, device_id_type=MESH)
    for e in LINE:
        pl.semaphore_signal(barrier, inc=1, device_id=other_core(*e), device_id_type=MESH)
        pl.semaphore_signal(barrier, inc=1, device_id=other_core(*e[::-1]), device_id_type=MESH)

    lane = lax.broadcasted_iota(jnp.int32, (16, 128), 1)
    left = lane < 64
    action = lax.broadcasted_iota(jnp.int32, (16, 128), 0)
    for copy in small:
        copy.wait()
    for s in range(16):
        rows = pl.ds(s * 16, 16)
        masked[0, rows, :] = jnp.where(action < counts[s], costs[rows, :], jnp.float32(BIG))

    pl.semaphore_wait(barrier, len(PARTNERS) + 1 + 2 * len(LINE))

    def to_partner(src, dst, k):
        copy = pltpu.make_async_remote_copy(
            src, dst, pair_send.at[k], pair_recv.at[k], device_id=partner, device_id_type=MESH
        )
        copy.start()
        return copy

    send_start = to_partner(start, swap.at[0], 0)
    send_cost = to_partner(masked.at[0], masked.at[1], 1)
    exchanges = []
    for i in range(4):
        rows = pl.ds(i * quarter, quarter)
        copy = pltpu.make_async_remote_copy(
            trans.at[rows],
            raw.at[1, rows],
            raw_send.at[i],
            raw_recv.at[i],
            device_id=partner,
            device_id_type=MESH,
        )
        copy.start()
        exchanges.append(copy)

    keep = jnp.logical_xor(left, c == 1)

    def both_halves(v):
        return jnp.where(keep[: v.shape[0]], v, pltpu.roll(v, 64, 1))

    send_start.wait_recv()
    left8 = lax.broadcasted_iota(jnp.int32, (8, 128), 1) < 64
    own = both_halves(start[...])
    other = both_halves(swap[0])
    own = jnp.where(left8, own[:8], own[8:])
    other = jnp.where(left8, other[:8], other[8:])
    values[0, here, 0:8, :] = jnp.where(c == 0, own, other)
    values[0, here, 8:16, :] = jnp.where(c == 0, other, own)

    def split_rows(which, base):
        def step(i, _):
            rows = pl.ds(pl.multiple_of(i * 16, 16), 16)
            out_rows = pl.ds(pl.multiple_of(base + i * 16, 16), 16)
            for g in range(32):
                v = raw[which, rows, g * 128 : (g + 1) * 128]
                h = v.astype(jnp.bfloat16)
                hi[g // ZS, g % ZS, out_rows, :] = h
                lo[g // ZS, g % ZS, out_rows, :] = (v - h.astype(jnp.float32)).astype(jnp.bfloat16)
            return 0

        lax.fori_loop(0, 16, step, 0)

    def receive_sem(t, d):
        if d in HOLDERS:
            return hold_recv.at[t, HOLDERS[d]]
        g0, g1 = group_of(d, 0), group_of(d, 1)
        return leaf_recv.at[t, g0 + c * (g1 - g0)]

    def hand_on(t, p, receivers):
        chunk = source(p)
        if p:
            wait_bytes(values.at[t, chunk], hold_recv.at[t, HOLDERS[p]])
        for d in receivers:
            pltpu.make_async_remote_copy(
                values.at[t, chunk],
                values.at[t, chunk],
                send_sem.at[t],
                receive_sem(t, d),
                device_id=member(*step(d, p)),
                device_id_type=MESH,
            ).start()

    def wait_bytes(ref, sem):
        pltpu.make_async_copy(ref, ref, sem).wait()

    def wait_group(t, i):
        for core in range(2):
            n = sum(group_of(d, core) == i for d in LEAVES)

            @pl.when(c == core)
            def _():
                if n:
                    wait_bytes(values.at[t, 0:n], leaf_recv.at[t, i])

    def multiply(t, i, base):
        blocks = []
        for (y0, z0), (y1, z1) in zip(GROUPS[0][i], GROUPS[1][i]):
            blocks.append((wrap(y + y0 + c * (y1 - y0), 4), wrap(z + z0 + c * (z1 - z0), ZS)))
        n = len(blocks)
        v = jnp.concatenate([values[t, pl.ds((k[0] * ZS + k[1]) * XS, XS)].reshape(64, 128) for k in blocks], axis=0) - base
        h = v.astype(jnp.bfloat16).astype(jnp.float32)
        r = v - h
        l_ = lax.broadcasted_iota(jnp.int32, v.shape, 1) < 64
        turned = pltpu.roll(jnp.where(l_, r, h), 64, 1)
        top = jnp.where(l_, h, turned).reshape(n * 8, 1, 8, 128)
        bottom = jnp.where(l_, turned, r).reshape(n * 8, 1, 8, 128)
        w = jnp.concatenate([top, bottom], axis=1).reshape(n * 128, 128).astype(jnp.bfloat16)
        rows = [half[k[0], k[1]] for half in (hi, lo) for k in blocks]
        part = jnp.dot(
            jnp.concatenate(rows, axis=1), jnp.concatenate([w, w], axis=0), preferred_element_type=jnp.float32
        )
        if i == 0:
            total[...] = part
        else:
            total[...] += part

    def finish_costs():
        send_cost.wait_recv()

        def step(i, _):
            for which in range(2):
                rows = pl.ds(pl.multiple_of(i * 16, 16), 16)
                base = (c if which == 0 else 1 - c) * 256
                cost2[pl.ds(pl.multiple_of(base + i * 16, 16), 16), :] = both_halves(masked[which, rows, :])
            return 0

        lax.fori_loop(0, 16, step, 0)

    row8 = lax.broadcasted_iota(jnp.int32, (8, 128), 0)
    lane8 = lax.broadcasted_iota(jnp.int32, (8, 128), 1)

    def iteration(t, _):
        hand_on(t, *TREE[0])

        @pl.when(t == 0)
        def _():
            for copy in loads:
                copy.wait()
            split_rows(0, c * 256)

        for p, receivers in TREE[1:]:
            hand_on(t, p, receivers)

        @pl.when(t == 0)
        def _():
            finish_costs()
            for copy in exchanges:
                copy.wait_recv()
            split_rows(1, (1 - c) * 256)

        packed = values[t, here]
        base = packed[0:1, :]
        base = jnp.where(lax.broadcasted_iota(jnp.int32, (1, 128), 1) < 64, base, pltpu.roll(base, 64, 1))

        for i in range(len(GROUPS[0])):
            wait_group(t, i)
            multiply(t, i, base)

        e = total[...]
        q = e + pltpu.roll(e, 64, 1) + cost2[...]
        best = jnp.min(q.reshape(32, 16, 128), axis=1) + base
        best_io[0] = best[:16]
        best_io[1] = best[16:]
        new = jnp.concatenate(
            [jnp.where(left8, best[0:8], best[8:16]), jnp.where(left8, best[16:24], best[24:32])], axis=0
        )
        values[t + 1, here] = new
        return 0

    lax.fori_loop(0, ITERS, iteration, 0)

    device = (y * ZS + z) * XS + x
    ids = device * 32 + lax.broadcasted_iota(jnp.int32, (16, 128), 0)
    picked = jnp.maximum(
        jnp.where(ids == ref_state[0], best_io[0], -BIG), jnp.where(ids + 16 == ref_state[0], best_io[1], -BIG)
    )
    ref_row = jnp.max(picked, axis=0, keepdims=True)

    def bounds_of(inc):
        up = jnp.max(inc, axis=0, keepdims=True)
        down = jnp.max(-inc, axis=0, keepdims=True)
        up = jnp.maximum(up, pltpu.roll(up, 64, 1))
        down = jnp.maximum(down, pltpu.roll(down, 64, 1))
        return jnp.where(lane8[:1] < 64, up, down)

    mine[0] = jnp.concatenate([bounds_of(values[ITERS, here] - values[ITERS - 1, here]), ref_row], axis=0)
    send_best = to_partner(best_io.at[1 - c], swap.at[1], 2)

    for da, dz in PLANE[::-1]:
        pltpu.make_async_remote_copy(
            mine.at[0],
            plane_in.at[da * ZS + dz - 1],
            send_sem.at[4],
            plane_recv.at[da * ZS + dz - 1],
            device_id=member(da, dz, 0),
            device_id_type=MESH,
        ).start()

    def increases(t, _):
        def block(i, carry):
            up, down = carry
            chunks = pl.ds(pl.multiple_of(i * 8, 8), 8)
            inc = values[t + 1, chunks] - values[t, chunks]
            inc = inc.reshape(16, 8, 128)
            return jnp.maximum(up, jnp.max(inc, axis=0)), jnp.maximum(down, jnp.max(-inc, axis=0))

        low = jnp.full((8, 128), -BIG, jnp.float32)
        up, down = lax.fori_loop(0, YS * ZS * XS // 8, block, (low, low))
        up = jnp.max(up, axis=0, keepdims=True)
        down = jnp.max(down, axis=0, keepdims=True)
        up = jnp.maximum(up, pltpu.roll(up, 64, 1))
        down = jnp.maximum(down, pltpu.roll(down, 64, 1))
        bounds[0] = jnp.where(row8 == t, jnp.where(lane8 < 64, up, down), bounds[0])
        return 0

    bounds[0] = jnp.full((8, 128), -BIG, jnp.float32)
    lax.fori_loop(0, ITERS - 1, increases, 0)
    send_bounds = to_partner(bounds.at[0], bounds.at[1], 3)
    top = mine[0]
    for da, dz in PLANE:
        pltpu.make_async_remote_copy(
            mine.at[0],
            plane_in.at[da * ZS + dz - 1],
            send_sem.at[4],
            plane_recv.at[da * ZS + dz - 1],
            device_id=partner,
            device_id_type=MESH,
        ).wait_recv()
        top = jnp.maximum(top, plane_in[da * ZS + dz - 1])
    mine[1] = top
    lines = []
    for db in (2, 1, 3):
        for k, device in enumerate((other_core(0, 0, db), member(0, 0, db))):
            copy = pltpu.make_async_remote_copy(
                mine.at[1],
                line_in.at[4 * k + db],
                line_send.at[4 * k + db],
                line_recv.at[4 * k + db],
                device_id=device,
                device_id_type=MESH,
            )
            copy.start()
            lines.append(copy)
    copy = pltpu.make_async_remote_copy(
        mine.at[1], line_in.at[0], line_send.at[0], line_recv.at[0], device_id=partner, device_id_type=MESH
    )
    copy.start()
    lines.append(copy)
    for copy in lines:
        copy.wait_recv()
    other = jnp.maximum(jnp.maximum(line_in[0], line_in[1]), jnp.maximum(line_in[2], line_in[3]))
    top = jnp.maximum(jnp.maximum(top, line_in[5]), jnp.maximum(line_in[6], line_in[7]))
    send_bounds.wait_recv()
    own_bounds = jnp.where(row8 == ITERS - 1, top[0:1], bounds[0])
    other_bounds = jnp.where(row8 == ITERS - 1, other[0:1], bounds[1])
    r0 = jnp.where(c == 0, own_bounds, other_bounds)
    r1 = jnp.where(c == 0, other_bounds, own_bounds)
    upper = jnp.where(left8, r0, pltpu.roll(r1, 64, 1))
    lower = -jnp.where(left8, pltpu.roll(r0, 64, 1), r1)
    ref_full = jnp.where(jnp.logical_xor(left8[:1], c == 1), top[1:2], other[1:2])
    out[16:20, :] = upper[0:4]
    out[20:24, :] = lower[0:4]
    send_best.wait_recv()
    out[0:16, :] = jnp.where(keep, jnp.where(c == 0, best_io[0], best_io[1]), swap[1]) - ref_full

    def sent(t, _):
        wait_bytes(values.at[t, 0:127], send_sem.at[t])
        return 0

    lax.fori_loop(0, ITERS, sent, 0)
    wait_bytes(plane_in.at[0:31], send_sem.at[4])
    for copy in (send_start, send_cost, send_best, send_bounds, *lines, *exchanges):
        copy.wait_send()


def deal(out, relative, lower, upper):
    relative[...] = out[0:16, :]
    upper[...] = out[16:20, :]
    lower[...] = out[20:24, :]


def local(transitions, costs, valid_counts, start_values, ref_state):
    dma = pltpu.SemaphoreType.DMA
    f32, bf16 = jnp.float32, jnp.bfloat16
    vmem = pl.BlockSpec(memory_space=pltpu.VMEM)
    out = pl.pallas_call(
        kernel,
        out_shape=jax.ShapeDtypeStruct((24, 128), f32),
        in_specs=[pl.BlockSpec(memory_space=pl.ANY)] * 5,
        out_specs=vmem,
        scratch_shapes=[
            pltpu.VMEM((ITERS + 1, YS * ZS * XS, 16, 128), f32),
            pltpu.VMEM((256, 128), f32),
            pltpu.SMEM((16,), jnp.int32),
            pltpu.VMEM((16, 128), f32),
            pltpu.SMEM((1,), jnp.int32),
            pltpu.VMEM((2, 256, 4096), f32),
            pltpu.VMEM((YS, ZS, 512, 128), bf16),
            pltpu.VMEM((YS, ZS, 512, 128), bf16),
            pltpu.VMEM((2, 256, 128), f32),
            pltpu.VMEM((512, 128), f32),
            pltpu.VMEM((512, 128), f32),
            pltpu.VMEM((2, 16, 128), f32),
            pltpu.VMEM((2, 2, 128), f32),
            pltpu.VMEM((4 * ZS - 1, 2, 128), f32),
            pltpu.VMEM((8, 2, 128), f32),
            pltpu.VMEM((2, 8, 128), f32),
            pltpu.VMEM((2, 16, 128), f32),
            dma((ITERS, len(TREE))),
            dma((ITERS, len(GROUPS[0]))),
            dma((4 * ZS - 1,)),
            dma((8,)),
            dma((ITERS + 1,)),
            dma((8,)),
            dma((4,)),
            dma((4,)),
            dma((4,)),
            dma((4,)),
            dma((4,)),
            dma((4,)),
        ],
        compiler_params=pltpu.CompilerParams(
            collective_id=0, has_side_effects=True, vmem_limit_bytes=60 * 1024 * 1024
        ),
        name="value_iteration",
    )(
        transitions.reshape(256, 4096),
        costs.reshape(256, 128),
        valid_counts,
        start_values,
        ref_state,
    )
    return pl.pallas_call(
        deal,
        out_shape=(
            jax.ShapeDtypeStruct((16, 128), f32),
            jax.ShapeDtypeStruct((ITERS, 128), f32),
            jax.ShapeDtypeStruct((ITERS, 128), f32),
        ),
        in_specs=[vmem],
        out_specs=(vmem, vmem, vmem),
        name="deal",
    )(out)


def solution(mesh):
    split = Mesh(mesh.devices.reshape(YS, ZS, XS, 2), AXES)
    return jax.shard_map(
        local,
        mesh=split,
        in_specs=(P(AXES, None, None), P(AXES, None, None), P(AXES), P(AXES, None), P()),
        out_specs=(P(AXES, None), P(), P()),
        check_vma=False,
    )
```

```python
import functools

import jax
import jax.numpy as jnp
from jax import lax
from jax.experimental import pallas as pl
from jax.experimental.pallas import tpu as pltpu
from jax.sharding import Mesh
from jax.sharding import PartitionSpec as P

ITERS = 4
YS, ZS, XS = 4, 8, 4
AXES = ("y", "z", "x", "c")
BIG = 1e30
MESH = pl.DeviceIdType.MESH


def ring(delta, size):
    return min(delta, size - delta)


PLANE = sorted(
    ((da, dz) for da in range(4) for dz in range(ZS) if da or dz),
    key=lambda d: (ring(d[0], 4) + ring(d[1], ZS), ring(d[1], ZS), d),
)

TREE = (
    (0, (11, 1, 28, 92, 4, 13, 94, 36, 20, 75, 25, 32, 33, 101, 79, 123, 16, 35, 10, 66, 99, 70, 116, 2, 96, 3, 22, 64, 125, 97, 37, 103, 68, 31)),
    (1, (34, 98, 30, 85, 65, 5)),
    (28, (127, 124, 29, 60, 61, 95, 56)),
    (4, (105, 69, 6, 100, 7, 102)),
    (32, (62,)),
    (96, (104, 67)),
    (36, (71, 40, 38)),
    (11, (106, 8, 111, 47, 15)),
    (33, (93,)),
    (20, (23, 24, 21)),
    (35, (63, 59, 39)),
    (25, (121, 26, 57, 58)),
    (13, (73, 81, 45, 110, 12, 49, 14, 113, 9, 44, 17, 46, 77, 109)),
    (116, (114, 118, 112, 120, 84, 115, 108, 117, 52)),
    (123, (90, 88, 119, 122, 27, 87, 91)),
    (75, (74, 43, 107, 72)),
    (125, (126, 89)),
    (37, (41,)),
    (10, (42,)),
    (79, (76, 83, 78, 80, 51, 82)),
    (22, (50, 86, 18, 54)),
    (56, (48, 55)),
    (15, (19,)),
    (21, (53,)),
)
GROUPS = (
    (
        ((0, 0), (3, 0), (0, 1), (1, 0), (0, 7), (2, 0), (0, 3), (2, 1)),
        ((3, 7), (0, 6), (2, 7), (3, 1), (1, 7), (3, 2), (0, 5), (0, 2), (1, 2), (1, 6), (1, 1), (1, 5), (3, 5), (2, 6), (1, 3), (3, 6)),
        ((2, 5), (1, 4), (2, 2), (2, 4), (2, 3), (0, 4), (3, 3), (3, 4)),
    ),
    (
        ((0, 0), (0, 1), (0, 7), (2, 0), (3, 0), (1, 0), (1, 1), (3, 1)),
        ((1, 7), (3, 7), (2, 7), (1, 5), (0, 6), (2, 1), (1, 2), (3, 5), (3, 4), (1, 6), (3, 6), (2, 6), (0, 5), (2, 5), (0, 2), (0, 3)),
        ((2, 2), (3, 2), (2, 3), (2, 4), (1, 3), (3, 3), (0, 4), (1, 4)),
    ),
)


def parts(d):
    return d // 32, d // 4 % ZS, d % 4


def step(d, p):
    return tuple((i - j) % n for i, j, n in zip(parts(d), parts(p), (4, ZS, 4)))


HOLDERS = {p: i for i, (p, _) in enumerate(TREE)}
LINE = ((0, 0, 2), (0, 0, 1), (0, 0, 3))
PARTNERS = sorted(
    {step(d, p) for p, receivers in TREE for d in receivers} | {(da, dz, 0) for da, dz in PLANE} | set(LINE)
)
PARTNERS = sorted(
    set(PARTNERS) | {tuple(-i % n for i, n in zip(e, (4, ZS, 4))) for e in PARTNERS},
    key=lambda e: (-sum(ring(i, n) for i, n in zip(e, (4, ZS, 4))), e),
)


def group_of(d, c):
    a, z, b = step(0, d)
    block = (a if c == 0 else b, z)
    return next(i for i, g in enumerate(GROUPS[c]) if block in g)


LEAVES = [d for d in range(1, 128) if d not in HOLDERS]


def kernel(
    trans,
    costs_in,
    counts_in,
    start_in,
    ref_in,
    out,
    values,
    costs,
    counts,
    start,
    ref_state,
    raw,
    hi,
    lo,
    masked,
    cost2,
    total,
    swap,
    mine,
    plane_in,
    line_in,
    bounds,
    best_io,
    hold_recv,
    leaf_recv,
    plane_recv,
    line_recv,
    send_sem,
    line_send,
    small_sem,
    raw_sem,
    raw_send,
    raw_recv,
    pair_send,
    pair_recv,
):
    y, z, x, c = (lax.axis_index(a) for a in AXES)
    a = y + c * (x - y)
    b = x + c * (y - x)

    def wrap(i, size):
        return lax.rem(i + size, size)

    def place(a_, z_, b_):
        y_ = a_ + c * (b_ - a_)
        x_ = b_ + c * (a_ - b_)
        return y_, z_, x_

    partner = (y, z, x, 1 - c)
    here = (y * ZS + z) * XS + x

    def member(da, dz, db):
        return (*place(wrap(a + da, 4), wrap(z + dz, ZS), wrap(b + db, 4)), c)

    def other_core(da, dz, db):
        return (*place(wrap(a + da, 4), wrap(z + dz, ZS), wrap(b + db, 4)), 1 - c)

    def source(d):
        da, dz, db = parts(d)
        y_, z_, x_ = place(wrap(a - da, 4), wrap(z - dz, ZS), wrap(b - db, 4))
        return (y_ * ZS + z_) * XS + x_

    small = []
    for i, (src, dst) in enumerate(
        ((start_in, start), (costs_in, costs), (counts_in, counts), (ref_in, ref_state))
    ):
        copy = pltpu.make_async_copy(src, dst, small_sem.at[i])
        copy.start()
        small.append(copy)
    quarter = 64
    loads = []
    for i in range(4):
        rows = pl.ds(i * quarter, quarter)
        copy = pltpu.make_async_copy(trans.at[rows], raw.at[0, rows], raw_sem.at[i])
        copy.start()
        loads.append(copy)

    barrier = pltpu.get_barrier_semaphore()
    for e in PARTNERS:
        pl.semaphore_signal(barrier, inc=1, device_id=member(*e), device_id_type=MESH)
    pl.semaphore_signal(barrier, inc=1, device_id=partner, device_id_type=MESH)
    for e in LINE:
        pl.semaphore_signal(barrier, inc=1, device_id=other_core(*e), device_id_type=MESH)
        pl.semaphore_signal(barrier, inc=1, device_id=other_core(*e[::-1]), device_id_type=MESH)

    lane = lax.broadcasted_iota(jnp.int32, (16, 128), 1)
    left = lane < 64
    action = lax.broadcasted_iota(jnp.int32, (16, 128), 0)
    for copy in small:
        copy.wait()
    for s in range(16):
        rows = pl.ds(s * 16, 16)
        masked[0, rows, :] = jnp.where(action < counts[s], costs[rows, :], jnp.float32(BIG))

    pl.semaphore_wait(barrier, len(PARTNERS) + 1 + 2 * len(LINE))

    def to_partner(src, dst, k):
        copy = pltpu.make_async_remote_copy(
            src, dst, pair_send.at[k], pair_recv.at[k], device_id=partner, device_id_type=MESH
        )
        copy.start()
        return copy

    send_start = to_partner(start, swap.at[0], 0)
    send_cost = to_partner(masked.at[0], masked.at[1], 1)
    exchanges = []
    for i in range(4):
        rows = pl.ds(i * quarter, quarter)
        copy = pltpu.make_async_remote_copy(
            trans.at[rows],
            raw.at[1, rows],
            raw_send.at[i],
            raw_recv.at[i],
            device_id=partner,
            device_id_type=MESH,
        )
        copy.start()
        exchanges.append(copy)

    keep = jnp.logical_xor(left, c == 1)

    def both_halves(v):
        return jnp.where(keep[: v.shape[0]], v, pltpu.roll(v, 64, 1))

    send_start.wait_recv()
    left8 = lax.broadcasted_iota(jnp.int32, (8, 128), 1) < 64
    own = both_halves(start[...])
    other = both_halves(swap[0])
    own = jnp.where(left8, own[:8], own[8:])
    other = jnp.where(left8, other[:8], other[8:])
    values[0, here, 0:8, :] = jnp.where(c == 0, own, other)
    values[0, here, 8:16, :] = jnp.where(c == 0, other, own)

    def split_rows(which, base):
        def step(i, _):
            rows = pl.ds(pl.multiple_of(i * 16, 16), 16)
            out_rows = pl.ds(pl.multiple_of(base + i * 16, 16), 16)
            for g in range(32):
                v = raw[which, rows, g * 128 : (g + 1) * 128]
                h = v.astype(jnp.bfloat16)
                hi[g // ZS, g % ZS, out_rows, :] = h
                lo[g // ZS, g % ZS, out_rows, :] = (v - h.astype(jnp.float32)).astype(jnp.bfloat16)
            return 0

        lax.fori_loop(0, 16, step, 0)

    def receive_sem(t, d):
        if d in HOLDERS:
            return hold_recv.at[t, HOLDERS[d]]
        g0, g1 = group_of(d, 0), group_of(d, 1)
        return leaf_recv.at[t, g0 + c * (g1 - g0)]

    def hand_on(t, p, receivers):
        chunk = source(p)
        if p:
            wait_bytes(values.at[t, chunk], hold_recv.at[t, HOLDERS[p]])
        for d in receivers:
            pltpu.make_async_remote_copy(
                values.at[t, chunk],
                values.at[t, chunk],
                send_sem.at[t],
                receive_sem(t, d),
                device_id=member(*step(d, p)),
                device_id_type=MESH,
            ).start()

    def wait_bytes(ref, sem):
        pltpu.make_async_copy(ref, ref, sem).wait()

    def wait_group(t, i):
        for core in range(2):
            n = sum(group_of(d, core) == i for d in LEAVES)

            @pl.when(c == core)
            def _():
                if n:
                    wait_bytes(values.at[t, 0:n], leaf_recv.at[t, i])

    def multiply(t, i, base):
        blocks = []
        for (y0, z0), (y1, z1) in zip(GROUPS[0][i], GROUPS[1][i]):
            blocks.append((wrap(y + y0 + c * (y1 - y0), 4), wrap(z + z0 + c * (z1 - z0), ZS)))
        n = len(blocks)
        v = jnp.concatenate([values[t, pl.ds((k[0] * ZS + k[1]) * XS, XS)].reshape(64, 128) for k in blocks], axis=0) - base
        h = v.astype(jnp.bfloat16).astype(jnp.float32)
        r = v - h
        l_ = lax.broadcasted_iota(jnp.int32, v.shape, 1) < 64
        turned = pltpu.roll(jnp.where(l_, r, h), 64, 1)
        top = jnp.where(l_, h, turned).reshape(n * 8, 1, 8, 128)
        bottom = jnp.where(l_, turned, r).reshape(n * 8, 1, 8, 128)
        w = jnp.concatenate([top, bottom], axis=1).reshape(n * 128, 128).astype(jnp.bfloat16)
        rows = [half[k[0], k[1]] for half in (hi, lo) for k in blocks]
        part = jnp.dot(
            jnp.concatenate(rows, axis=1), jnp.concatenate([w, w], axis=0), preferred_element_type=jnp.float32
        )
        if i == 0:
            total[...] = part
        else:
            total[...] += part

    def finish_costs():
        send_cost.wait_recv()

        def step(i, _):
            for which in range(2):
                rows = pl.ds(pl.multiple_of(i * 16, 16), 16)
                base = (c if which == 0 else 1 - c) * 256
                cost2[pl.ds(pl.multiple_of(base + i * 16, 16), 16), :] = both_halves(masked[which, rows, :])
            return 0

        lax.fori_loop(0, 16, step, 0)

    row8 = lax.broadcasted_iota(jnp.int32, (8, 128), 0)
    lane8 = lax.broadcasted_iota(jnp.int32, (8, 128), 1)

    def iteration(t, _):
        hand_on(t, *TREE[0])

        @pl.when(t == 0)
        def _():
            for copy in loads:
                copy.wait()
            split_rows(0, c * 256)

        for p, receivers in TREE[1:]:
            hand_on(t, p, receivers)

        @pl.when(t == 0)
        def _():
            finish_costs()
            for copy in exchanges:
                copy.wait_recv()
            split_rows(1, (1 - c) * 256)

        packed = values[t, here]
        base = packed[0:1, :]
        base = jnp.where(lax.broadcasted_iota(jnp.int32, (1, 128), 1) < 64, base, pltpu.roll(base, 64, 1))

        for i in range(len(GROUPS[0])):
            wait_group(t, i)
            multiply(t, i, base)

        e = total[...]
        q = e + pltpu.roll(e, 64, 1) + cost2[...]
        best = jnp.min(q.reshape(32, 16, 128), axis=1) + base
        best_io[0] = best[:16]
        best_io[1] = best[16:]
        new = jnp.concatenate(
            [jnp.where(left8, best[0:8], best[8:16]), jnp.where(left8, best[16:24], best[24:32])], axis=0
        )
        values[t + 1, here] = new
        return 0

    lax.fori_loop(0, ITERS, iteration, 0)

    device = (y * ZS + z) * XS + x
    ids = device * 32 + lax.broadcasted_iota(jnp.int32, (16, 128), 0)
    picked = jnp.maximum(
        jnp.where(ids == ref_state[0], best_io[0], -BIG), jnp.where(ids + 16 == ref_state[0], best_io[1], -BIG)
    )
    ref_row = jnp.max(picked, axis=0, keepdims=True)

    def bounds_of(inc):
        up = jnp.max(inc, axis=0, keepdims=True)
        down = jnp.max(-inc, axis=0, keepdims=True)
        up = jnp.maximum(up, pltpu.roll(up, 64, 1))
        down = jnp.maximum(down, pltpu.roll(down, 64, 1))
        return jnp.where(lane8[:1] < 64, up, down)

    mine[0] = jnp.concatenate([bounds_of(values[ITERS, here] - values[ITERS - 1, here]), ref_row], axis=0)
    send_best = to_partner(best_io.at[1 - c], swap.at[1], 2)

    for da, dz in PLANE[::-1]:
        pltpu.make_async_remote_copy(
            mine.at[0],
            plane_in.at[da * ZS + dz - 1],
            send_sem.at[4],
            plane_recv.at[da * ZS + dz - 1],
            device_id=member(da, dz, 0),
            device_id_type=MESH,
        ).start()

    def increases(t, _):
        def block(i, carry):
            up, down = carry
            chunks = pl.ds(pl.multiple_of(i * 8, 8), 8)
            inc = values[t + 1, chunks] - values[t, chunks]
            inc = inc.reshape(16, 8, 128)
            return jnp.maximum(up, jnp.max(inc, axis=0)), jnp.maximum(down, jnp.max(-inc, axis=0))

        low = jnp.full((8, 128), -BIG, jnp.float32)
        up, down = lax.fori_loop(0, YS * ZS * XS // 8, block, (low, low))
        up = jnp.max(up, axis=0, keepdims=True)
        down = jnp.max(down, axis=0, keepdims=True)
        up = jnp.maximum(up, pltpu.roll(up, 64, 1))
        down = jnp.maximum(down, pltpu.roll(down, 64, 1))
        bounds[0] = jnp.where(row8 == t, jnp.where(lane8 < 64, up, down), bounds[0])
        return 0

    bounds[0] = jnp.full((8, 128), -BIG, jnp.float32)
    lax.fori_loop(0, ITERS - 1, increases, 0)
    send_bounds = to_partner(bounds.at[0], bounds.at[1], 3)
    top = mine[0]
    for da, dz in PLANE:
        pltpu.make_async_remote_copy(
            mine.at[0],
            plane_in.at[da * ZS + dz - 1],
            send_sem.at[4],
            plane_recv.at[da * ZS + dz - 1],
            device_id=partner,
            device_id_type=MESH,
        ).wait_recv()
        top = jnp.maximum(top, plane_in[da * ZS + dz - 1])
    mine[1] = top
    lines = []
    for db in (2, 1, 3):
        for k, device in enumerate((other_core(0, 0, db), member(0, 0, db))):
            copy = pltpu.make_async_remote_copy(
                mine.at[1],
                line_in.at[4 * k + db],
                line_send.at[4 * k + db],
                line_recv.at[4 * k + db],
                device_id=device,
                device_id_type=MESH,
            )
            copy.start()
            lines.append(copy)
    copy = pltpu.make_async_remote_copy(
        mine.at[1], line_in.at[0], line_send.at[0], line_recv.at[0], device_id=partner, device_id_type=MESH
    )
    copy.start()
    lines.append(copy)
    for copy in lines:
        copy.wait_recv()
    other = jnp.maximum(jnp.maximum(line_in[0], line_in[1]), jnp.maximum(line_in[2], line_in[3]))
    top = jnp.maximum(jnp.maximum(top, line_in[5]), jnp.maximum(line_in[6], line_in[7]))
    send_bounds.wait_recv()
    own_bounds = jnp.where(row8 == ITERS - 1, top[0:1], bounds[0])
    other_bounds = jnp.where(row8 == ITERS - 1, other[0:1], bounds[1])
    r0 = jnp.where(c == 0, own_bounds, other_bounds)
    r1 = jnp.where(c == 0, other_bounds, own_bounds)
    upper = jnp.where(left8, r0, pltpu.roll(r1, 64, 1))
    lower = -jnp.where(left8, pltpu.roll(r0, 64, 1), r1)
    ref_full = jnp.where(jnp.logical_xor(left8[:1], c == 1), top[1:2], other[1:2])
    out[16:20, :] = upper[0:4]
    out[20:24, :] = lower[0:4]
    send_best.wait_recv()
    out[0:16, :] = jnp.where(keep, jnp.where(c == 0, best_io[0], best_io[1]), swap[1]) - ref_full

    def sent(t, _):
        wait_bytes(values.at[t, 0:127], send_sem.at[t])
        return 0

    lax.fori_loop(0, ITERS, sent, 0)
    wait_bytes(plane_in.at[0:31], send_sem.at[4])
    for copy in (send_start, send_cost, send_best, send_bounds, *lines, *exchanges):
        copy.wait_send()


def deal(out, relative, lower, upper):
    relative[...] = out[0:16, :]
    upper[...] = out[16:20, :]
    lower[...] = out[20:24, :]


def local(transitions, costs, valid_counts, start_values, ref_state):
    dma = pltpu.SemaphoreType.DMA
    f32, bf16 = jnp.float32, jnp.bfloat16
    vmem = pl.BlockSpec(memory_space=pltpu.VMEM)
    out = pl.pallas_call(
        kernel,
        out_shape=jax.ShapeDtypeStruct((24, 128), f32),
        in_specs=[pl.BlockSpec(memory_space=pl.ANY)] * 5,
        out_specs=vmem,
        scratch_shapes=[
            pltpu.VMEM((ITERS + 1, YS * ZS * XS, 16, 128), f32),
            pltpu.VMEM((256, 128), f32),
            pltpu.SMEM((16,), jnp.int32),
            pltpu.VMEM((16, 128), f32),
            pltpu.SMEM((1,), jnp.int32),
            pltpu.VMEM((2, 256, 4096), f32),
            pltpu.VMEM((YS, ZS, 512, 128), bf16),
            pltpu.VMEM((YS, ZS, 512, 128), bf16),
            pltpu.VMEM((2, 256, 128), f32),
            pltpu.VMEM((512, 128), f32),
            pltpu.VMEM((512, 128), f32),
            pltpu.VMEM((2, 16, 128), f32),
            pltpu.VMEM((2, 2, 128), f32),
            pltpu.VMEM((4 * ZS - 1, 2, 128), f32),
            pltpu.VMEM((8, 2, 128), f32),
            pltpu.VMEM((2, 8, 128), f32),
            pltpu.VMEM((2, 16, 128), f32),
            dma((ITERS, len(TREE))),
            dma((ITERS, len(GROUPS[0]))),
            dma((4 * ZS - 1,)),
            dma((8,)),
            dma((ITERS + 1,)),
            dma((8,)),
            dma((4,)),
            dma((4,)),
            dma((4,)),
            dma((4,)),
            dma((4,)),
            dma((4,)),
        ],
        compiler_params=pltpu.CompilerParams(
            collective_id=0, has_side_effects=True, vmem_limit_bytes=60 * 1024 * 1024
        ),
        name="value_iteration",
    )(
        transitions.reshape(256, 4096),
        costs.reshape(256, 128),
        valid_counts,
        start_values,
        ref_state,
    )
    return pl.pallas_call(
        deal,
        out_shape=(
            jax.ShapeDtypeStruct((16, 128), f32),
            jax.ShapeDtypeStruct((ITERS, 128), f32),
            jax.ShapeDtypeStruct((ITERS, 128), f32),
        ),
        in_specs=[vmem],
        out_specs=(vmem, vmem, vmem),
        name="deal",
    )(out)


def solution(mesh):
    split = Mesh(mesh.devices.reshape(YS, ZS, XS, 2), AXES)
    return jax.shard_map(
        local,
        mesh=split,
        in_specs=(P(AXES, None, None), P(AXES, None, None), P(AXES), P(AXES, None), P()),
        out_specs=(P(AXES, None), P(), P()),
        check_vma=False,
    )
```
